32 devices in a mesh: beam: 2 (over x), gx: 16 (over z, y, core).
Axes of the slice: x: 2, y: 2, z: 4, core: 2. Of those that a mesh axis runs over, the one named last changes fastest.
Arguments:
- filterbank: bfloat16 [4096, 2048], P(('beam', 'gx')), parts along dimension 0, may hold values from -61 to 61
- chan_delay: int32 [16, 2048], P(None, 'gx'), may hold values from 0 to 7
- sub_delay: int32 [1536, 64], replicated, may hold values from 0 to 15
- widths: int32 [1536], replicated, may hold values from 1 to 16
Outputs:
- snr: float32 [3072, 2048], P('beam', 'gx'), parts along dimension 0
The draws below stay inside these ranges and needn't reach their ends.
There are 2 independent parts, one for each index of `beam`. The reference program is written for one: setup_inputs(seed, part) draws one part's arguments, and reference() takes and returns one part's arrays. A program takes and returns all parts, laid end to end along the dimension named above; an argument that names none is the same for every part. Nothing has to cross between parts.
All inputs are finite; a program needn't handle non-finite values.
Results may differ from the reference program's by a relative error of at most 0.00059.
Values may be sent and summed in bfloat16 or wider, within the bound.
No kernel may reach another device: no remote copies, remote signals or barrier semaphores. Data moves between devices by JAX's collectives and lax.ppermute only.
A program may use at most 128 MiB of HBM per device.

```python
import math
import jax
import jax.numpy as jnp
from jax import lax

SUBCH = 32
CHANS = 2048
NSUB = 64
SAMPLES = 2048
GROUPS = 16
PER_GROUP = 96
TRIALS = 1536
DELAY_ONE = 8
DELAY_TWO = 16
WMAX = 16


def draw_filterbank(key, part):
    base = jax.random.fold_in(key, 11)
    key_band, key_noise = jax.random.split(base, 2)
    time_ramp = 1.0 + 2.0 * jnp.arange(SAMPLES, dtype=jnp.float32) / (SAMPLES - 1)
    bandpass = jnp.exp(jax.random.uniform(key_band, (CHANS, 1), jnp.float32, math.log(0.5), math.log(2.0)))
    noise = jax.random.truncated_normal(key_noise, -6.0, 6.0, (CHANS, SAMPLES), jnp.float32)
    return (bandpass * time_ramp[None, :] * (noise + 0.05)).astype(jnp.bfloat16)


def place_ends(entries, stream_key, least, top_value):
    place = [jax.random.randint(jax.random.fold_in(stream_key, axis), (), 0, length) for axis, length in enumerate(entries.shape)]
    main_axis = entries.shape.index(max(entries.shape))
    neighbour = place[:main_axis] + [(place[main_axis] + 1) % entries.shape[main_axis]] + place[main_axis + 1:]
    return entries.at[tuple(place)].set(least).at[tuple(neighbour)].set(top_value)


def setup_inputs(seed: int = 0, part: int = 0) -> dict:
    key_of = jax.random.split(jax.random.key(seed), 5)
    part_keys = jax.random.split(jax.random.fold_in(key_of[4], part), 5)
    filterbank = draw_filterbank(jax.random.fold_in(jax.random.fold_in(key_of[4], part), 71), part)
    chan_delay = place_ends(jax.random.randint(key_of[1], (GROUPS, CHANS), 0, DELAY_ONE), jax.random.fold_in(key_of[1], 1), 0, DELAY_ONE - 1).astype(jnp.int32)
    sub_delay = place_ends(jax.random.randint(key_of[2], (TRIALS, NSUB), 0, DELAY_TWO), jax.random.fold_in(key_of[2], 1), 0, DELAY_TWO - 1).astype(jnp.int32)
    widths = place_ends(jax.random.randint(key_of[3], (TRIALS,), 1, WMAX + 1), jax.random.fold_in(key_of[3], 1), 1, WMAX).astype(jnp.int32)
    return dict(filterbank=filterbank, chan_delay=chan_delay, sub_delay=sub_delay, widths=widths)


def band_sum(inputs):
    band_rows, delay_rows = inputs

    def per_group(delay_line):
        return jax.vmap(lambda series_row, offset: lax.dynamic_slice_in_dim(series_row, offset, SAMPLES))(band_rows, delay_line)
    shifted = jax.vmap(per_group)(delay_rows)
    return lax.optimization_barrier(jnp.sum(shifted.astype(jnp.float32), axis=1)).astype(jnp.bfloat16)

def reference(filterbank, chan_delay, sub_delay, widths):
    padded = jnp.pad(filterbank, ((0, 0), (0, DELAY_ONE)))
    band_input = padded.reshape(NSUB, SUBCH, SAMPLES + DELAY_ONE)
    band_delays = jnp.transpose(chan_delay.reshape(GROUPS, NSUB, SUBCH), (1, 0, 2))
    subbands = lax.map(band_sum, (band_input, band_delays))
    subbands_pad = jnp.pad(subbands, ((0, 0), (0, 0), (0, DELAY_TWO)))

    def trial_series(inputs):
        trial_index, delay_line = inputs
        group_rows = lax.dynamic_index_in_dim(subbands_pad, trial_index // PER_GROUP, 1, keepdims=False)
        shifted = jax.vmap(lambda series_row, offset: lax.dynamic_slice_in_dim(series_row, offset, SAMPLES))(group_rows, delay_line)
        return lax.optimization_barrier(jnp.sum(shifted.astype(jnp.float32), axis=0))
    series = lax.map(trial_series, (jnp.arange(TRIALS, dtype=jnp.int32), sub_delay))
    average = lax.optimization_barrier(jnp.sum(series, axis=1)) / SAMPLES
    variance = lax.optimization_barrier(jnp.sum((series - average[:, None]) ** 2, axis=1)) / SAMPLES
    padded_series = jnp.pad(series, ((0, 0), (0, WMAX)))
    boxcar = jnp.zeros((TRIALS, SAMPLES), jnp.float32)
    for offset in range(WMAX):
        boxcar = boxcar + jnp.where(offset < widths[:, None], padded_series[:, offset:offset + SAMPLES], 0.0)
    width_float = widths.astype(jnp.float32)[:, None]
    return (boxcar - width_float * average[:, None]) / jnp.sqrt(width_float * (variance[:, None] + 1e-05))
```

```python
import functools

import jax
import jax.numpy as jnp
from jax import lax
from jax.experimental import pallas as pl
from jax.experimental.pallas import tpu as pltpu
from jax.sharding import PartitionSpec as P

SUBCH = 32
DELAY_ONE = 8
DELAY_TWO = 16
WMAX = 16
LANES = 128
HALO = 32


def band_kernel(sub_count, groups, fb_ref, delay_ref, out_ref, rolled, tile):
    slabs = out_ref.shape[0]
    rows = sub_count * groups
    width = 2 * LANES
    chunks = slabs // 2
    delays = delay_ref[...]
    band_of = lax.broadcasted_iota(jnp.int32, delays.shape, 1) // SUBCH
    hot = []
    for offset in range(DELAY_ONE):
        for band in range(sub_count):
            hot.append(jnp.where((delays == offset) & (band_of == band), 1.0, 0.0))
    hot = jnp.concatenate(hot, 0).astype(jnp.bfloat16)
    lane = lax.broadcasted_iota(jnp.int32, (rows, width), 1)
    quarter = lax.broadcasted_iota(jnp.int32, (rows // 4, LANES), 1) // HALO
    out_ref[slabs - 1, rows:, :] = jnp.zeros((rows // 4, LANES), out_ref.dtype)
    rolled[lax.rem(chunks, 2)] = jnp.zeros(rolled.shape[1:], rolled.dtype)

    def body(i, carry):
        chunk = chunks - 1 - i
        now, later = lax.rem(chunk, 2), lax.rem(chunk + 1, 2)
        start = pl.multiple_of(chunk * width, width)
        parts = jnp.dot(hot, fb_ref[:, pl.ds(start, width)], preferred_element_type=jnp.float32)
        total = parts[:rows]
        for offset in range(1, DELAY_ONE):
            turned = pltpu.roll(parts[offset * rows : (offset + 1) * rows], width - offset, 1)
            following = jnp.concatenate([turned[:, :LANES], rolled[later, offset - 1]], 1)
            rolled[now, offset - 1] = turned[:, LANES:]
            total = total + jnp.where(lane < width - offset, turned, following)
        total = total.astype(jnp.bfloat16)
        for half in range(2):
            part = total[:, half * LANES : (half + 1) * LANES]
            slab = chunk * 2 + half
            out_ref[slab, :rows, :] = part
            tile[...] = part.astype(jnp.float32)
            packed = tile[pl.ds(0, rows // 4, 4), :]
            for q in range(1, 4):
                piece = pltpu.roll(tile[pl.ds(q, rows // 4, 4), :], HALO * q, 1)
                packed = jnp.where(quarter == q, piece, packed)
            packed = packed.astype(out_ref.dtype)
            if half:
                out_ref[slab - 1, rows:, :] = packed
            else:
                @pl.when(chunk > 0)
                def _():
                    out_ref[slab - 1, rows:, :] = packed
        return carry

    lax.fori_loop(0, chunks, body, 0)


def band_stage(filterbank, chan_delay, slabs):
    groups = chan_delay.shape[0]
    sub_count = filterbank.shape[0] // SUBCH
    rows = sub_count * groups
    return pl.pallas_call(
        functools.partial(band_kernel, sub_count, groups),
        out_shape=jax.ShapeDtypeStruct((slabs, rows + rows // 4, LANES), jnp.bfloat16),
        scratch_shapes=[
            pltpu.VMEM((2, DELAY_ONE - 1, rows, LANES), jnp.float32),
            pltpu.VMEM((rows, LANES), jnp.float32),
        ],
        name="bands",
    )(filterbank, chan_delay)


def trial_kernel(groups, per_group, held_ref, delay_ref, width_ref, box_ref, stat_ref, wide, slid, delays_at, series, stats):
    sources, row_count, _ = held_ref.shape
    bands, trials = delay_ref.shape
    per_source = bands // sources
    rows = per_source * groups
    blocks = trials // LANES
    copies = max(1, LANES // bands)
    span = LANES + WMAX
    base = 8
    rows = per_source * groups
    for block in range(blocks):
        delays_at[block] = delay_ref[:, block * LANES : (block + 1) * LANES]
    wide[...] = held_ref[...].reshape(sources * row_count, LANES).astype(jnp.float32)

    def turned(first_row, stride):
        picked = [
            wide[pl.ds(first_row + part * stride, sources, row_count), :] for part in range(per_source)
        ]
        return jnp.concatenate(picked * copies, 0).T

    def store(group, first, block):
        slid[group, base + first : base + first + block.shape[0], :] = block

    def store_slid(group, first, block):
        for copy in range(1, copies):
            low = copy * bands
            top = low + bands
            begin = base + first - copy
            slid[group, begin : begin + block.shape[0], low:top] = block[:, low:top]

    def spread(quad, carry):
        tails = turned(rows + quad, groups // 4)
        for q in range(4):
            group = quad * 4 + q
            body = turned(group, groups)
            tail = tails[q * HALO : (q + 1) * HALO]
            store(group, 0, body)
            store(group, LANES, tail)
            store_slid(group, 0, body)
            store_slid(group, LANES, tail)
        return carry

    lax.fori_loop(0, groups // 4, spread, 0)

    lane = lax.broadcasted_iota(jnp.int32, (span, LANES), 1)
    period = per_group // 32
    starts = [LANES * m // per_group for m in range(period)]
    splits = [per_group * (g + 1) - LANES * m for m, g in enumerate(starts)]

    def group_rows(group, offset):
        return slid[group, base + offset : base + offset + span, :]

    def cycle(turn, carry):
        for part in range(period):
            block = turn * period + part
            first_group = turn * (period * LANES // per_group) + starts[part]
            delays = jnp.concatenate(
                [delays_at[block, pl.ds(b, sources, per_source), :] for b in range(per_source)], 0
            )
            left = jnp.zeros((span, LANES), jnp.float32)
            right = jnp.zeros((span, LANES), jnp.float32)
            step = 2 * copies
            for offset in range(0, DELAY_TWO, step):
                hot = jnp.concatenate(
                    [jnp.where(delays == offset + e, 1.0, 0.0) for e in range(step)], 0
                )
                pieces = range(offset, offset + step, copies)
                left_rows = jnp.concatenate([group_rows(first_group, o) for o in pieces], 1)
                right_rows = jnp.concatenate([group_rows(first_group + 1, o) for o in pieces], 1)
                left = left + jnp.dot(left_rows, hot, preferred_element_type=jnp.float32)
                right = right + jnp.dot(right_rows, hot, preferred_element_type=jnp.float32)
            whole = jnp.where(lane < splits[part], left, right)
            series[...] = whole
            own = whole[:LANES]
            total = jnp.sum(own, 0, keepdims=True)
            centred = own - total * (1.0 / LANES)
            stats[pl.ds(block, 1), :] = total
            stats[pl.ds(blocks + block, 1), :] = jnp.sum(centred * centred, 0, keepdims=True)
            width = width_ref[pl.ds(block, 1), :]
            box = own
            for offset in range(1, WMAX):
                box = box + jnp.where(width > offset, series[offset : offset + LANES, :], 0.0)
            box_ref[block] = box
        return carry

    lax.fori_loop(0, blocks // period, cycle, 0)
    stat_ref[...] = jnp.broadcast_to(stats[...][None], stat_ref.shape)


def trial_stage(held, delays, widths, groups):
    sources, row_count, _ = held.shape
    bands, trials = delays.shape
    blocks = trials // LANES
    across = max(LANES, bands)
    return pl.pallas_call(
        functools.partial(trial_kernel, groups, trials // groups),
        out_shape=(
            jax.ShapeDtypeStruct((blocks, LANES, LANES), jnp.float32),
            jax.ShapeDtypeStruct((sources, 2 * blocks, LANES), jnp.float32),
        ),
        scratch_shapes=[
            pltpu.VMEM((sources * row_count, LANES), jnp.float32),
            pltpu.VMEM((groups, LANES + HALO + 8, across), jnp.float32),
            pltpu.VMEM((blocks, bands, LANES), jnp.int32),
            pltpu.VMEM((LANES + WMAX, LANES), jnp.float32),
            pltpu.VMEM((2 * blocks, LANES), jnp.float32),
        ],
        name="trials",
    )(held, delays, widths)


def snr_kernel(samples, box_ref, stat_ref, width_ref, out_ref):
    sources = stat_ref.shape[0]
    blocks = box_ref.shape[0]
    own = samples // sources
    totals = stat_ref[:, :blocks, :]
    average = jnp.sum(totals, 0) * (1.0 / samples)
    apart = totals * (1.0 / own) - average[None]
    squares = jnp.sum(stat_ref[:, blocks:, :], 0) + own * jnp.sum(apart * apart, 0)
    variance = squares * (1.0 / samples)
    width = width_ref[...].astype(jnp.float32)
    scale = 1.0 / jnp.sqrt(width * (variance + 1e-05))
    level = width * average
    for block in range(blocks):
        value = (box_ref[block] - level[block : block + 1]) * scale[block : block + 1]
        out_ref[block * LANES : (block + 1) * LANES, :] = value.T


def snr_stage(box, stats, widths, samples):
    blocks = box.shape[0]
    return pl.pallas_call(
        functools.partial(snr_kernel, samples),
        out_shape=jax.ShapeDtypeStruct((blocks * LANES, LANES), jnp.float32),
        name="snr",
    )(box, stats, widths)


def per_device(filterbank, chan_delay, sub_delay, widths):
    samples = filterbank.shape[1]
    groups = chan_delay.shape[0]
    slabs = lax.axis_size("gx")
    widths = widths.reshape(-1, LANES)
    sent = band_stage(filterbank, chan_delay, slabs)
    held = lax.all_to_all(sent, "gx", split_axis=0, concat_axis=0, tiled=True)
    box, stats = trial_stage(held, sub_delay.T, widths, groups)
    stats = lax.all_to_all(stats, "gx", split_axis=0, concat_axis=0, tiled=True)
    return snr_stage(box, stats, widths, samples)


def solution(mesh):
    in_specs = (P(("beam", "gx"), None), P(None, "gx"), P(), P())
    out_specs = P("beam", "gx")
    return jax.shard_map(
        per_device, mesh=mesh, in_specs=in_specs, out_specs=out_specs, check_vma=False
    )
```

```python
import functools
import math

import jax
import jax.numpy as jnp
from jax import lax
from jax.experimental import pallas as pl
from jax.experimental.pallas import tpu as pltpu
from jax.sharding import PartitionSpec as P

SUBCH = 32
DELAY_ONE = 8
DELAY_TWO = 16
WMAX = 16
LANES = 128
HALO = 32
NEAR = 4


def band_kernel(sub_count, groups, run, fb_hbm, delay_hbm, out_ref, held, delays_ref, carry, tile, sems):
    slabs = out_ref.shape[0]
    channels, samples = fb_hbm.shape
    rows = sub_count * groups
    fetch_delays = pltpu.make_async_copy(delay_hbm, delays_ref, sems.at[0])
    fetch = pltpu.make_async_copy(fb_hbm, held.at[:, :samples], sems.at[1])
    fetch_delays.start()
    fetch.start()
    held[:, samples:] = jnp.zeros((channels, LANES), held.dtype)
    carry[...] = jnp.zeros(carry.shape, carry.dtype)
    out_ref[slabs - 1, rows:, :] = jnp.zeros((rows // 4, LANES), out_ref.dtype)
    fetch_delays.wait()
    delays = delays_ref[...]
    band_of = lax.broadcasted_iota(jnp.int32, delays.shape, 1) // SUBCH
    hot = []
    for far in range(0, DELAY_ONE, NEAR):
        for band in range(sub_count):
            hot.append(
                jnp.concatenate(
                    [
                        jnp.where((delays == far + near) & (band_of == band), 1.0, 0.0)
                        for near in range(NEAR)
                    ],
                    1,
                )
            )
    hot = jnp.concatenate(hot, 0).astype(jnp.bfloat16)
    lane = lax.broadcasted_iota(jnp.int32, (channels, LANES), 1)
    out_lane = lax.broadcasted_iota(jnp.int32, (rows, LANES), 1)
    quarter = lax.broadcasted_iota(jnp.int32, (rows // 4, LANES), 1) // HALO
    fetch.wait()

    def turn(i, _):
        first = (slabs // run - 1 - i) * run

        def tile_at(j):
            return held[:, pl.ds(pl.multiple_of((first + j) * LANES, LANES), LANES)]

        def turned_all(j):
            block = tile_at(j)
            return [block] + [pltpu.roll(block, LANES - near, 1) for near in range(1, NEAR)]

        following = turned_all(run)
        late = carry[...]
        for pair in range(run // 2 - 1, -1, -1):
            sides = [None, None]
            for half in (1, 0):
                here = turned_all(2 * pair + half)
                sides[half] = jnp.concatenate(
                    [here[0]]
                    + [
                        jnp.where(lane < LANES - near, here[near], following[near])
                        for near in range(1, NEAR)
                    ],
                    0,
                )
                following = here
            parts = jnp.dot(hot, jnp.concatenate(sides, 1), preferred_element_type=jnp.float32)
            for half in (1, 0):
                part = parts[:, half * LANES : (half + 1) * LANES]
                total = part[:rows]
                fresh = pltpu.roll(part[rows:], LANES - NEAR, 1)
                total = total + jnp.where(out_lane < LANES - NEAR, fresh, late)
                late = fresh
                total = total.astype(jnp.bfloat16)
                slot = 2 * pair + half
                slab = first + slot
                out_ref[slab, :rows, :] = total
                tile[slot] = total.astype(jnp.float32)
                packed = tile[slot, pl.ds(0, rows // 4, 4), :]
                for q in range(1, 4):
                    piece = pltpu.roll(tile[slot, pl.ds(q, rows // 4, 4), :], HALO * q, 1)
                    packed = jnp.where(quarter == q, piece, packed)
                packed = packed.astype(out_ref.dtype)
                if slot:
                    out_ref[slab - 1, rows:, :] = packed
                else:
                    @pl.when(slab > 0)
                    def _():
                        out_ref[slab - 1, rows:, :] = packed
        carry[...] = late
        return 0

    if run == slabs:
        turn(0, 0)
    else:
        lax.fori_loop(0, slabs // run, turn, 0)


def band_stage(filterbank, chan_delay, slabs):
    groups = chan_delay.shape[0]
    channels, samples = filterbank.shape
    rows = channels // SUBCH * groups
    run = math.gcd(slabs, 16)
    return pl.pallas_call(
        functools.partial(band_kernel, channels // SUBCH, groups, run),
        out_shape=jax.ShapeDtypeStruct((slabs, rows + rows // 4, LANES), jnp.bfloat16),
        in_specs=[pl.BlockSpec(memory_space=pltpu.HBM)] * 2,
        scratch_shapes=[
            pltpu.VMEM((channels, samples + LANES), jnp.bfloat16),
            pltpu.VMEM(chan_delay.shape, jnp.int32),
            pltpu.VMEM((rows, LANES), jnp.float32),
            pltpu.VMEM((run, rows, LANES), jnp.float32),
            pltpu.SemaphoreType.DMA((2,)),
        ],
        compiler_params=pltpu.CompilerParams(vmem_limit_bytes=(8 << 20) + 2 * filterbank.size),
        name="bands",
    )(*(pltpu.with_memory_space_constraint(x, pltpu.HBM) for x in (filterbank, chan_delay)))


def trial_kernel(groups, per_group, held_ref, delay_ref, width_ref, box_ref, stat_ref, wide, slid, delays_at, series, stats):
    sources, row_count, _ = held_ref.shape
    bands, trials = delay_ref.shape
    per_source = bands // sources
    rows = per_source * groups
    blocks = trials // LANES
    copies = max(1, LANES // bands)
    span = LANES + WMAX
    base = 8
    rows = per_source * groups
    for block in range(blocks):
        delays_at[block] = delay_ref[:, block * LANES : (block + 1) * LANES]
    wide[...] = held_ref[...].reshape(sources * row_count, LANES).astype(jnp.float32)

    def turned(first_row, stride):
        picked = [
            wide[pl.ds(first_row + part * stride, sources, row_count), :] for part in range(per_source)
        ]
        return jnp.concatenate(picked * copies, 0).T

    def store(group, first, block):
        slid[group, base + first : base + first + block.shape[0], :] = block

    def store_slid(group, first, block):
        for copy in range(1, copies):
            low = copy * bands
            top = low + bands
            begin = base + first - copy
            slid[group, begin : begin + block.shape[0], low:top] = block[:, low:top]

    def spread(quad, carry):
        tails = turned(rows + quad, groups // 4)
        for q in range(4):
            group = quad * 4 + q
            body = turned(group, groups)
            tail = tails[q * HALO : (q + 1) * HALO]
            store(group, 0, body)
            store(group, LANES, tail)
            store_slid(group, 0, body)
            store_slid(group, LANES, tail)
        return carry

    lax.fori_loop(0, groups // 4, spread, 0)

    lane = lax.broadcasted_iota(jnp.int32, (span, LANES), 1)
    period = per_group // 32
    starts = [LANES * m // per_group for m in range(period)]
    splits = [per_group * (g + 1) - LANES * m for m, g in enumerate(starts)]

    def group_rows(group, offset):
        return slid[group, base + offset : base + offset + span, :]

    def cycle(turn, carry):
        for part in range(period):
            block = turn * period + part
            first_group = turn * (period * LANES // per_group) + starts[part]
            delays = jnp.concatenate(
                [delays_at[block, pl.ds(b, sources, per_source), :] for b in range(per_source)], 0
            )
            left = jnp.zeros((span, LANES), jnp.float32)
            right = jnp.zeros((span, LANES), jnp.float32)
            step = 2 * copies
            for offset in range(0, DELAY_TWO, step):
                hot = jnp.concatenate(
                    [jnp.where(delays == offset + e, 1.0, 0.0) for e in range(step)], 0
                )
                pieces = range(offset, offset + step, copies)
                left_rows = jnp.concatenate([group_rows(first_group, o) for o in pieces], 1)
                right_rows = jnp.concatenate([group_rows(first_group + 1, o) for o in pieces], 1)
                left = left + jnp.dot(left_rows, hot, preferred_element_type=jnp.float32)
                right = right + jnp.dot(right_rows, hot, preferred_element_type=jnp.float32)
            whole = jnp.where(lane < splits[part], left, right)
            series[...] = whole
            own = whole[:LANES]
            total = jnp.sum(own, 0, keepdims=True)
            centred = own - total * (1.0 / LANES)
            stats[pl.ds(block, 1), :] = total
            stats[pl.ds(blocks + block, 1), :] = jnp.sum(centred * centred, 0, keepdims=True)
            width = width_ref[pl.ds(block, 1), :]
            box = own
            for offset in range(1, WMAX):
                box = box + jnp.where(width > offset, series[offset : offset + LANES, :], 0.0)
            box_ref[block] = box
        return carry

    lax.fori_loop(0, blocks // period, cycle, 0)
    stat_ref[...] = jnp.broadcast_to(stats[...][None], stat_ref.shape)


def trial_stage(held, delays, widths, groups):
    sources, row_count, _ = held.shape
    bands, trials = delays.shape
    blocks = trials // LANES
    across = max(LANES, bands)
    return pl.pallas_call(
        functools.partial(trial_kernel, groups, trials // groups),
        out_shape=(
            jax.ShapeDtypeStruct((blocks, LANES, LANES), jnp.float32),
            jax.ShapeDtypeStruct((sources, 2 * blocks, LANES), jnp.float32),
        ),
        scratch_shapes=[
            pltpu.VMEM((sources * row_count, LANES), jnp.float32),
            pltpu.VMEM((groups, LANES + HALO + 8, across), jnp.float32),
            pltpu.VMEM((blocks, bands, LANES), jnp.int32),
            pltpu.VMEM((LANES + WMAX, LANES), jnp.float32),
            pltpu.VMEM((2 * blocks, LANES), jnp.float32),
        ],
        compiler_params=pltpu.CompilerParams(vmem_limit_bytes=(8 << 20) + 8 * DELAY_TWO * delays.size),
        name="trials",
    )(held, delays, widths)


def snr_kernel(samples, box_ref, stat_ref, width_ref, out_ref):
    sources = stat_ref.shape[0]
    blocks = box_ref.shape[0]
    own = samples // sources
    totals = stat_ref[:, :blocks, :]
    average = jnp.sum(totals, 0) * (1.0 / samples)
    apart = totals * (1.0 / own) - average[None]
    squares = jnp.sum(stat_ref[:, blocks:, :], 0) + own * jnp.sum(apart * apart, 0)
    variance = squares * (1.0 / samples)
    width = width_ref[...].astype(jnp.float32)
    scale = 1.0 / jnp.sqrt(width * (variance + 1e-05))
    level = width * average
    for block in range(blocks):
        value = (box_ref[block] - level[block : block + 1]) * scale[block : block + 1]
        out_ref[block * LANES : (block + 1) * LANES, :] = value.T


def snr_stage(box, stats, widths, samples):
    blocks = box.shape[0]
    return pl.pallas_call(
        functools.partial(snr_kernel, samples),
        out_shape=jax.ShapeDtypeStruct((blocks * LANES, LANES), jnp.float32),
        compiler_params=pltpu.CompilerParams(vmem_limit_bytes=8 << 20),
        name="snr",
    )(box, stats, widths)


def per_device(filterbank, chan_delay, sub_delay, widths):
    samples = filterbank.shape[1]
    groups = chan_delay.shape[0]
    slabs = lax.axis_size("gx")
    widths = widths.reshape(-1, LANES)
    sent = band_stage(filterbank, chan_delay, slabs)
    held = lax.all_to_all(sent, "gx", split_axis=0, concat_axis=0, tiled=True)
    box, stats = trial_stage(held, sub_delay.T, widths, groups)
    stats = lax.all_to_all(stats, "gx", split_axis=0, concat_axis=0, tiled=True)
    return snr_stage(box, stats, widths, samples)


def solution(mesh):
    in_specs = (P(("beam", "gx"), None), P(None, "gx"), P(), P())
    out_specs = P("beam", "gx")
    return jax.shard_map(
        per_device, mesh=mesh, in_specs=in_specs, out_specs=out_specs, check_vma=False
    )
```

```python
import functools
import math

import jax
import jax.numpy as jnp
from jax import lax
from jax.experimental import pallas as pl
from jax.experimental.pallas import tpu as pltpu
from jax.sharding import PartitionSpec as P

SUBCH = 32
DELAY_ONE = 8
DELAY_TWO = 16
WMAX = 16
LANES = 128
HALO = 32
NEAR = 4
COST = pl.CostEstimate(flops=1 << 28, bytes_accessed=1 << 20, transcendentals=0)


def band_kernel(sub_count, groups, run, fb_hbm, delay_hbm, out_ref, held, delays_ref, carry, tile, sems):
    slabs = out_ref.shape[0]
    channels, samples = fb_hbm.shape
    rows = sub_count * groups
    fetch_delays = pltpu.make_async_copy(delay_hbm, delays_ref, sems.at[0])
    fetch = pltpu.make_async_copy(fb_hbm, held.at[:, :samples], sems.at[1])
    fetch_delays.start()
    fetch.start()
    held[:, samples:] = jnp.zeros((channels, LANES), held.dtype)
    carry[...] = jnp.zeros(carry.shape, carry.dtype)
    out_ref[slabs - 1, rows:, :] = jnp.zeros((rows // 4, LANES), out_ref.dtype)
    fetch_delays.wait()
    delays = delays_ref[...]
    band_of = lax.broadcasted_iota(jnp.int32, delays.shape, 1) // SUBCH
    hot = []
    for far in range(0, DELAY_ONE, NEAR):
        for band in range(sub_count):
            hot.append(
                jnp.concatenate(
                    [
                        jnp.where((delays == far + near) & (band_of == band), 1.0, 0.0)
                        for near in range(NEAR)
                    ],
                    1,
                )
            )
    hot = jnp.concatenate(hot, 0).astype(jnp.bfloat16)
    lane = lax.broadcasted_iota(jnp.int32, (channels, LANES), 1)
    out_lane = lax.broadcasted_iota(jnp.int32, (rows, LANES), 1)
    quarter = lax.broadcasted_iota(jnp.int32, (rows // 4, LANES), 1) // HALO
    fetch.wait()

    def turn(i, _):
        first = (slabs // run - 1 - i) * run

        def tile_at(j):
            return held[:, pl.ds(pl.multiple_of((first + j) * LANES, LANES), LANES)]

        def turned_all(j):
            block = tile_at(j)
            return [block] + [pltpu.roll(block, LANES - near, 1) for near in range(1, NEAR)]

        following = turned_all(run)
        late = carry[...]
        for pair in range(run // 2 - 1, -1, -1):
            sides = [None, None]
            for half in (1, 0):
                here = turned_all(2 * pair + half)
                sides[half] = jnp.concatenate(
                    [here[0]]
                    + [
                        jnp.where(lane < LANES - near, here[near], following[near])
                        for near in range(1, NEAR)
                    ],
                    0,
                )
                following = here
            parts = jnp.dot(hot, jnp.concatenate(sides, 1), preferred_element_type=jnp.float32)
            for half in (1, 0):
                part = parts[:, half * LANES : (half + 1) * LANES]
                total = part[:rows]
                fresh = pltpu.roll(part[rows:], LANES - NEAR, 1)
                total = total + jnp.where(out_lane < LANES - NEAR, fresh, late)
                late = fresh
                total = total.astype(jnp.bfloat16)
                slot = 2 * pair + half
                slab = first + slot
                out_ref[slab, :rows, :] = total
                tile[slot] = total.astype(jnp.float32)
                packed = tile[slot, pl.ds(0, rows // 4, 4), :]
                for q in range(1, 4):
                    piece = pltpu.roll(tile[slot, pl.ds(q, rows // 4, 4), :], HALO * q, 1)
                    packed = jnp.where(quarter == q, piece, packed)
                packed = packed.astype(out_ref.dtype)
                if slot:
                    out_ref[slab - 1, rows:, :] = packed
                else:
                    @pl.when(slab > 0)
                    def _():
                        out_ref[slab - 1, rows:, :] = packed
        carry[...] = late
        return 0

    if run == slabs:
        turn(0, 0)
    else:
        lax.fori_loop(0, slabs // run, turn, 0)


def band_stage(filterbank, chan_delay, slabs):
    groups = chan_delay.shape[0]
    channels, samples = filterbank.shape
    rows = channels // SUBCH * groups
    run = math.gcd(slabs, 16)
    return pl.pallas_call(
        functools.partial(band_kernel, channels // SUBCH, groups, run),
        out_shape=jax.ShapeDtypeStruct((slabs, rows + rows // 4, LANES), jnp.bfloat16),
        in_specs=[pl.BlockSpec(memory_space=pltpu.HBM)] * 2,
        scratch_shapes=[
            pltpu.VMEM((channels, samples + LANES), jnp.bfloat16),
            pltpu.VMEM(chan_delay.shape, jnp.int32),
            pltpu.VMEM((rows, LANES), jnp.float32),
            pltpu.VMEM((run, rows, LANES), jnp.float32),
            pltpu.SemaphoreType.DMA((2,)),
        ],
        compiler_params=pltpu.CompilerParams(vmem_limit_bytes=(8 << 20) + 2 * filterbank.size),
        name="bands",
    )(*(pltpu.with_memory_space_constraint(x, pltpu.HBM) for x in (filterbank, chan_delay)))


def group_lanes(row_pair, group, per_group):
    start = group * per_group
    first, shift = start // LANES, start % LANES
    if not shift:
        return row_pair(first)
    front = pltpu.roll(row_pair(first), LANES - shift, 1)
    if shift + per_group <= LANES:
        return front
    back = pltpu.roll(row_pair(first + 1), LANES - shift, 1)
    lane = lax.broadcasted_iota(jnp.int32, front.shape, 1)
    return jnp.where(lane < LANES - shift, front, back)


def one_hot(delays, first, count):
    return jnp.concatenate([jnp.where(delays == first + e, 1.0, 0.0) for e in range(count)], 0)


def pieces_of(per_group):
    period = per_group // HALO
    starts = [LANES * m // per_group for m in range(period)]
    splits = [per_group * (g + 1) - LANES * m for m, g in enumerate(starts)]
    return period, starts, splits


def series_kernel(whole, per_group, held_ref, delay_ref, series_ref, stat_ref, wide, slid, dense, near, rows_at):
    sources, row_count, _ = held_ref.shape
    groups = series_ref.shape[0]
    bands, trials = delay_ref.shape
    per_source = bands // sources
    rows = per_source * groups
    pitch = row_count + 1
    copies = max(1, LANES // bands)
    span = LANES + WMAX
    base = 8
    for block in range(trials // LANES):
        dense[block] = delay_ref[:, block * LANES : (block + 1) * LANES]

    def ordered(block):
        return jnp.concatenate(
            [dense[block, pl.ds(b, sources, per_source), :] for b in range(per_source)], 0
        )

    for group in range(groups):
        near[group] = group_lanes(ordered, group, per_group)
    for source in range(sources):
        wide[source * pitch : source * pitch + row_count, :] = held_ref[source].astype(jnp.float32)

    def turned(first_row, stride):
        picked = [
            wide[pl.ds(first_row + part * stride, sources, pitch), :] for part in range(per_source)
        ]
        return jnp.concatenate(picked * copies, 0).T

    def store(q, first, block):
        slid[q, base + first : base + first + block.shape[0], :] = block

    def store_slid(q, first, block):
        for copy in range(1, copies):
            low = copy * bands
            top = low + bands
            begin = base + first - copy
            slid[q, begin : begin + block.shape[0], low:top] = block[:, low:top]

    def quad_of(quad, at):
        tails = turned(rows + quad, groups // 4)
        for q in range(4):
            group = quad * 4 + q
            place = at + q
            body = turned(group, groups)
            tail = tails[q * HALO : (q + 1) * HALO]
            store(place, 0, body)
            store(place, LANES, tail)
            store_slid(place, 0, body)
            store_slid(place, LANES, tail)
            out = jnp.zeros((span, LANES), jnp.float32)
            step = 2 * copies
            for offset in range(0, DELAY_TWO, step):
                hot = one_hot(near[group], offset, step)
                left = jnp.concatenate(
                    [
                        slid[place, base + o : base + o + span, :]
                        for o in range(offset, offset + step, copies)
                    ],
                    1,
                )
                out = out + jnp.dot(left, hot, preferred_element_type=jnp.float32)
            series_ref[group] = out
            own = out[:LANES]
            total = jnp.sum(own, 0, keepdims=True)
            centred = own - total * (1.0 / LANES)
            rows_at[0, pl.ds(group, 1), :] = total
            rows_at[1, pl.ds(group, 1), :] = jnp.sum(centred * centred, 0, keepdims=True)

    if whole:
        for quad in range(groups // 4):
            quad_of(quad, quad * 4)
    else:

        def turn(quad, _):
            quad_of(quad, 0)
            return 0

        lax.fori_loop(0, groups // 4, turn, 0)

    period, starts, splits = pieces_of(per_group)
    cycle = period + 1
    lane = lax.broadcasted_iota(jnp.int32, (groups // cycle, LANES), 1)
    packed = []
    for stat in range(2):
        moved = [rows_at[stat, pl.ds(q, groups // cycle, cycle), :] for q in range(cycle)]
        moved = [pltpu.roll(r, q * per_group % LANES, 1) if q else r for q, r in enumerate(moved)]
        for start, split in zip(starts, splits):
            packed.append(jnp.where(lane < split, moved[start], moved[start + 1]))
    packed = jnp.concatenate(packed, 0)
    stat_ref[...] = jnp.broadcast_to(packed[None], stat_ref.shape)


def series_stage(held, delays, groups):
    sources, row_count, _ = held.shape
    bands, trials = delays.shape
    across = max(LANES, bands)
    whole = bands <= LANES
    return pl.pallas_call(
        functools.partial(series_kernel, whole, trials // groups),
        out_shape=(
            jax.ShapeDtypeStruct((groups, LANES + WMAX, LANES), jnp.float32),
            jax.ShapeDtypeStruct((sources, 2 * trials // LANES, LANES), jnp.float32),
        ),
        scratch_shapes=[
            pltpu.VMEM((sources * (row_count + 1) + 7, LANES), jnp.float32),
            pltpu.VMEM((groups if whole else 4, LANES + HALO + 8, across), jnp.float32),
            pltpu.VMEM((trials // LANES, bands, LANES), jnp.int32),
            pltpu.VMEM((groups, bands, LANES), jnp.int32),
            pltpu.VMEM((2, groups, LANES), jnp.float32),
        ],
        compiler_params=pltpu.CompilerParams(vmem_limit_bytes=(8 << 20) + (0 if whole else 32 << 20)),
        name="series",
    )(held, delays)


def box_kernel(per_group, series_ref, width_ref, out_ref):
    groups = series_ref.shape[0]
    period, starts, splits = pieces_of(per_group)
    cycle = period + 1
    lane = lax.broadcasted_iota(jnp.int32, (LANES, LANES), 1)
    for turn in range(groups // cycle):
        moved = []
        for q in range(cycle):
            group = turn * cycle + q
            width = group_lanes(lambda r: width_ref[r : r + 1, :], group, per_group)
            box = series_ref[group, :LANES, :]
            for offset in range(1, WMAX):
                box = box + jnp.where(
                    width > offset, series_ref[group, offset : offset + LANES, :], 0.0
                )
            moved.append(pltpu.roll(box, q * per_group % LANES, 1) if q else box)
        for j, (start, split) in enumerate(zip(starts, splits)):
            out_ref[turn * period + j] = jnp.where(lane < split, moved[start], moved[start + 1])


def box_stage(series, widths, per_group):
    blocks = widths.shape[0]
    return pl.pallas_call(
        functools.partial(box_kernel, per_group),
        out_shape=jax.ShapeDtypeStruct((blocks, LANES, LANES), jnp.float32),
        compiler_params=pltpu.CompilerParams(vmem_limit_bytes=8 << 20),
        cost_estimate=COST,
        name="box",
    )(series, widths)


def snr_kernel(samples, period, box_ref, stat_ref, width_ref, out_hbm, done, sems):
    sources, stat_rows, _ = stat_ref.shape
    blocks = stat_rows // 2
    turns = blocks // period
    own = samples // sources
    totals = stat_ref[:, :blocks, :]
    average = jnp.sum(totals, 0) * (1.0 / samples)
    apart = totals * (1.0 / own) - average[None]
    squares = jnp.sum(stat_ref[:, blocks:, :], 0) + own * jnp.sum(apart * apart, 0)
    variance = squares * (1.0 / samples)
    width = jnp.concatenate([width_ref[pl.ds(j, turns, period), :] for j in range(period)], 0)
    width = width.astype(jnp.float32)
    scale = 1.0 / jnp.sqrt(width * (variance + 1e-05))
    level = width * average
    copies = []
    for turn in range(turns):
        for j in range(period):
            row = j * turns + turn
            block = turn * period + j
            value = (box_ref[block] - level[row : row + 1]) * scale[row : row + 1]
            done[block * LANES : (block + 1) * LANES, :] = value.T
        span = slice(turn * period * LANES, (turn + 1) * period * LANES)
        copy = pltpu.make_async_copy(done.at[span, :], out_hbm.at[span, :], sems.at[turn])
        copy.start()
        copies.append(copy)
    for copy in copies:
        copy.wait()


def snr_stage(box, stats, widths, samples, period):
    blocks = widths.shape[0]
    turns = blocks // period
    return pl.pallas_call(
        functools.partial(snr_kernel, samples, period),
        out_shape=jax.ShapeDtypeStruct((blocks * LANES, LANES), jnp.float32),
        out_specs=pl.BlockSpec(memory_space=pltpu.HBM),
        scratch_shapes=[
            pltpu.VMEM((blocks * LANES, LANES), jnp.float32),
            pltpu.SemaphoreType.DMA((turns,)),
        ],
        compiler_params=pltpu.CompilerParams(vmem_limit_bytes=8 << 20),
        name="snr",
    )(box, stats, widths)


def per_device(filterbank, chan_delay, sub_delay, widths):
    samples = filterbank.shape[1]
    groups = chan_delay.shape[0]
    per_group = sub_delay.shape[0] // groups
    slabs = lax.axis_size("gx")
    widths = widths.reshape(-1, LANES)
    sent = band_stage(filterbank, chan_delay, slabs)
    held = lax.all_to_all(sent, "gx", split_axis=0, concat_axis=0, tiled=True)
    series, stats = series_stage(held, sub_delay.T, groups)
    box = box_stage(series, widths, per_group)
    stats = lax.all_to_all(stats, "gx", split_axis=0, concat_axis=0, tiled=True)
    return snr_stage(box, stats, widths, samples, pieces_of(per_group)[0])


def solution(mesh):
    in_specs = (P(("beam", "gx"), None), P(None, "gx"), P(), P())
    out_specs = P("beam", "gx")
    return jax.shard_map(
        per_device, mesh=mesh, in_specs=in_specs, out_specs=out_specs, check_vma=False
    )
```

```python
import functools
import math

import jax
import jax.numpy as jnp
from jax import lax
from jax.experimental import pallas as pl
from jax.experimental.pallas import tpu as pltpu
from jax.sharding import PartitionSpec as P

SUBCH = 32
DELAY_ONE = 8
DELAY_TWO = 16
WMAX = 16
LANES = 128
HALO = 32
NEAR = 4
FAR = DELAY_TWO // 2
FETCHES = 1
PACE = 16
COST = pl.CostEstimate(flops=1 << 28, bytes_accessed=1 << 20, transcendentals=0)


def band_kernel(sub_count, groups, run, fb_hbm, delay_hbm, out_ref, held, delays_ref, carry, tile, sems):
    slabs = out_ref.shape[0]
    channels, samples = fb_hbm.shape
    rows = sub_count * groups
    fetch_delays = pltpu.make_async_copy(delay_hbm, delays_ref, sems.at[0])
    piece = samples // FETCHES
    fetches = [
        pltpu.make_async_copy(
            fb_hbm.at[:, p * piece : (p + 1) * piece],
            held.at[:, p * piece : (p + 1) * piece],
            sems.at[p + 1],
        )
        for p in range(FETCHES)
    ]
    fetch_delays.start()
    for fetch in reversed(fetches):
        fetch.start()
    held[:, samples:] = jnp.zeros((channels, LANES), held.dtype)
    carry[...] = jnp.zeros(carry.shape, carry.dtype)
    out_ref[slabs - 1, rows:, :] = jnp.zeros((rows // 4, LANES), out_ref.dtype)
    fetch_delays.wait()
    delays = delays_ref[...]
    band_of = lax.broadcasted_iota(jnp.int32, delays.shape, 1) // SUBCH
    hot = []
    for far in range(0, DELAY_ONE, NEAR):
        for band in range(sub_count):
            hot.append(
                jnp.concatenate(
                    [
                        jnp.where((delays == far + near) & (band_of == band), 1.0, 0.0)
                        for near in range(NEAR)
                    ],
                    1,
                )
            )
    hot = jnp.concatenate(hot, 0).astype(jnp.bfloat16)
    lane = lax.broadcasted_iota(jnp.int32, (channels, LANES), 1)
    out_lane = lax.broadcasted_iota(jnp.int32, (rows, LANES), 1)
    place = lax.broadcasted_iota(jnp.int32, (4 * LANES, LANES), 0)
    place_out = lax.broadcasted_iota(jnp.int32, (4 * LANES, LANES), 1)
    fold = (place % LANES < HALO) & (place // LANES * HALO + place % LANES == place_out)
    fold = jnp.where(fold, 1.0, 0.0)
    for fetch in fetches:
        fetch.wait()

    pace = math.gcd(run, PACE)

    def turn(i, _):
        first = (slabs // run - 1 - i) * run

        def tile_at(j):
            return held[:, pl.ds(pl.multiple_of((first + j) * LANES, LANES), LANES)]

        def turned_all(j):
            block = tile_at(j)
            return [block] + [pltpu.roll(block, LANES - near, 1) for near in range(1, NEAR)]

        following = turned_all(run)
        late = carry[...]
        for pack in range(run // pace - 1, -1, -1):
            sides = [None] * pace
            for side in range(pace - 1, -1, -1):
                here = turned_all(pace * pack + side)
                sides[side] = jnp.concatenate(
                    [here[0]]
                    + [
                        jnp.where(lane < LANES - near, here[near], following[near])
                        for near in range(1, NEAR)
                    ],
                    0,
                )
                following = here
            parts = jnp.dot(hot, jnp.concatenate(sides, 1), preferred_element_type=jnp.float32)
            for side in range(pace - 1, -1, -1):
                part = parts[:, side * LANES : (side + 1) * LANES]
                total = part[:rows]
                fresh = pltpu.roll(part[rows:], LANES - NEAR, 1)
                total = total + jnp.where(out_lane < LANES - NEAR, fresh, late)
                late = fresh
                total = total.astype(jnp.bfloat16)
                slot = pace * pack + side
                out_ref[first + slot, :rows, :] = total
                tile[slot * rows : (slot + 1) * rows, :] = total.astype(jnp.float32)
        ends = jnp.concatenate(
            [tile[pl.ds(q, run * rows // 4, 4), :] for q in range(4)], 1
        )
        ends = jnp.dot(ends, fold, preferred_element_type=jnp.float32).astype(out_ref.dtype)
        for slot in range(run):
            end = ends[slot * rows // 4 : (slot + 1) * rows // 4]
            if slot:
                out_ref[first + slot - 1, rows:, :] = end
            else:
                @pl.when(first > 0)
                def _():
                    out_ref[first - 1, rows:, :] = end
        carry[...] = late
        return 0

    if run == slabs:
        turn(0, 0)
    else:
        lax.fori_loop(0, slabs // run, turn, 0)


def band_stage(filterbank, chan_delay, slabs):
    groups = chan_delay.shape[0]
    channels, samples = filterbank.shape
    rows = channels // SUBCH * groups
    run = math.gcd(slabs, 16)
    return pl.pallas_call(
        functools.partial(band_kernel, channels // SUBCH, groups, run),
        out_shape=jax.ShapeDtypeStruct((slabs, rows + rows // 4, LANES), jnp.bfloat16),
        in_specs=[pl.BlockSpec(memory_space=pltpu.HBM)] * 2,
        scratch_shapes=[
            pltpu.VMEM((channels, samples + LANES), jnp.bfloat16),
            pltpu.VMEM(chan_delay.shape, jnp.int32),
            pltpu.VMEM((rows, LANES), jnp.float32),
            pltpu.VMEM((run * rows, LANES), jnp.float32),
            pltpu.SemaphoreType.DMA((FETCHES + 1,)),
        ],
        compiler_params=pltpu.CompilerParams(vmem_limit_bytes=(8 << 20) + 2 * filterbank.size),
        name="bands",
    )(*(pltpu.with_memory_space_constraint(x, pltpu.HBM) for x in (filterbank, chan_delay)))


def group_lanes(row_pair, group, per_group):
    start = group * per_group
    first, shift = start // LANES, start % LANES
    if not shift:
        return row_pair(first)
    front = pltpu.roll(row_pair(first), LANES - shift, 1)
    if shift + per_group <= LANES:
        return front
    back = pltpu.roll(row_pair(first + 1), LANES - shift, 1)
    lane = lax.broadcasted_iota(jnp.int32, front.shape, 1)
    return jnp.where(lane < LANES - shift, front, back)


def one_hot(delays, first, count):
    return jnp.concatenate([jnp.where(delays == first + e, 1.0, 0.0) for e in range(count)], 0)


def pieces_of(per_group):
    period = per_group // HALO
    starts = [LANES * m // per_group for m in range(period)]
    splits = [per_group * (g + 1) - LANES * m for m, g in enumerate(starts)]
    return period, starts, splits


def series_kernel(whole, per_group, held_ref, delay_ref, series_ref, stat_ref, wide, slid, dense, near, rows_at):
    sources, row_count, _ = held_ref.shape
    groups = series_ref.shape[0]
    bands, trials = delay_ref.shape
    per_source = bands // sources
    rows = per_source * groups
    pitch = row_count + 1
    copies = max(1, LANES // bands)
    span = LANES + WMAX
    base = 8
    for block in range(trials // LANES):
        dense[block] = delay_ref[:, block * LANES : (block + 1) * LANES]

    def ordered(block):
        return jnp.concatenate(
            [dense[block, pl.ds(b, sources, per_source), :] for b in range(per_source)], 0
        )

    for group in range(groups):
        near[group] = group_lanes(ordered, group, per_group)
    for source in range(sources):
        wide[source * pitch : source * pitch + row_count, :] = held_ref[source].astype(jnp.float32)

    def turned(first_row, stride):
        picked = [
            wide[pl.ds(first_row + part * stride, sources, pitch), :] for part in range(per_source)
        ]
        return jnp.concatenate(picked * copies, 0).T

    def store(q, first, block):
        slid[q, base + first : base + first + block.shape[0], :] = block

    def store_slid(q, first, block):
        for copy in range(1, copies):
            low = copy * bands
            top = low + bands
            begin = base + first - copy
            slid[q, begin : begin + block.shape[0], low:top] = block[:, low:top]

    def quad_of(quad, at):
        tails = turned(rows + quad, groups // 4)
        for q in range(4):
            group = quad * 4 + q
            place = at + q
            body = turned(group, groups)
            tail = tails[q * HALO : (q + 1) * HALO]
            store(place, 0, body)
            store(place, LANES, tail)
            store_slid(place, 0, body)
            store_slid(place, LANES, tail)
            both = jnp.zeros((span + FAR, 2 * LANES), jnp.float32)
            step = 2 * copies
            for offset in range(0, FAR, step):
                hot = jnp.concatenate(
                    [one_hot(near[group], far + offset, step) for far in (0, FAR)], 1
                )
                left = jnp.concatenate(
                    [
                        slid[place, base + o : base + o + span + FAR, :]
                        for o in range(offset, offset + step, copies)
                    ],
                    1,
                )
                both = both + jnp.dot(left, hot, preferred_element_type=jnp.float32)
            out = both[:span, :LANES] + both[FAR:, LANES:]
            series_ref[group] = out
            own = out[:LANES]
            total = jnp.sum(own, 0, keepdims=True)
            centred = own - total * (1.0 / LANES)
            rows_at[0, pl.ds(group, 1), :] = total
            rows_at[1, pl.ds(group, 1), :] = jnp.sum(centred * centred, 0, keepdims=True)

    if whole:
        for quad in range(groups // 4):
            quad_of(quad, quad * 4)
    else:

        def turn(quad, _):
            quad_of(quad, 0)
            return 0

        lax.fori_loop(0, groups // 4, turn, 0)

    period, starts, splits = pieces_of(per_group)
    cycle = period + 1
    lane = lax.broadcasted_iota(jnp.int32, (groups // cycle, LANES), 1)
    packed = []
    for stat in range(2):
        moved = [rows_at[stat, pl.ds(q, groups // cycle, cycle), :] for q in range(cycle)]
        moved = [pltpu.roll(r, q * per_group % LANES, 1) if q else r for q, r in enumerate(moved)]
        for start, split in zip(starts, splits):
            packed.append(jnp.where(lane < split, moved[start], moved[start + 1]))
    stat_ref[...] = jnp.concatenate(packed, 0)


def series_stage(held, delays, groups):
    sources, row_count, _ = held.shape
    bands, trials = delays.shape
    across = max(LANES, bands)
    whole = bands <= LANES
    return pl.pallas_call(
        functools.partial(series_kernel, whole, trials // groups),
        out_shape=(
            jax.ShapeDtypeStruct((groups, LANES + WMAX, LANES), jnp.float32),
            jax.ShapeDtypeStruct((2 * trials // LANES, LANES), jnp.float32),
        ),
        scratch_shapes=[
            pltpu.VMEM((sources * (row_count + 1) + 7, LANES), jnp.float32),
            pltpu.VMEM((groups if whole else 4, LANES + HALO + 8, across), jnp.float32),
            pltpu.VMEM((trials // LANES, bands, LANES), jnp.int32),
            pltpu.VMEM((groups, bands, LANES), jnp.int32),
            pltpu.VMEM((2, groups, LANES), jnp.float32),
        ],
        compiler_params=pltpu.CompilerParams(vmem_limit_bytes=(8 << 20) + (0 if whole else 32 << 20)),
        name="series",
    )(held, delays)


def box_kernel(per_group, series_ref, width_ref, out_ref, pairs, ones, fours, threes):
    groups = series_ref.shape[0]
    period, starts, splits = pieces_of(per_group)
    cycle = period + 1
    lane = lax.broadcasted_iota(jnp.int32, (LANES, LANES), 1)

    def window(ref, group, first, count):
        return ref[group, first : first + count, :]

    def boxes(group):
        width = group_lanes(lambda r: width_ref[r : r + 1, :], group, per_group)
        bits = [width & (1 << e) > 0 for e in range(5)]
        top = LANES + 15
        here = window(series_ref, group, 0, top)
        pairs[group, :top, :] = here + window(series_ref, group, 1, top)
        ones[group, :top, :] = jnp.where(bits[0], here, 0.0)
        top = LANES + 12
        two = window(pairs, group, 0, top)
        fours[group, :top, :] = two + window(pairs, group, 2, top)
        threes[group, :top, :] = jnp.where(
            bits[1], two + window(ones, group, 2, top), window(ones, group, 0, top)
        )
        top = LANES + 8
        four = window(fours, group, 0, top)
        eight = four + window(fours, group, 4, top)
        seven = jnp.where(
            bits[2], four + window(threes, group, 4, top), window(threes, group, 0, top)
        )
        part = jnp.where(bits[3], eight[:LANES] + seven[8:], seven[:LANES])
        return jnp.where(bits[4], eight[:LANES] + eight[8:], part)

    for turn in range(groups // cycle):
        moved = []
        for q in range(cycle):
            box = boxes(turn * cycle + q)
            moved.append(pltpu.roll(box, q * per_group % LANES, 1) if q else box)
        for j, (start, split) in enumerate(zip(starts, splits)):
            out_ref[turn * period + j] = jnp.where(lane < split, moved[start], moved[start + 1])


def box_stage(series, widths, per_group):
    blocks = widths.shape[0]
    return pl.pallas_call(
        functools.partial(box_kernel, per_group),
        out_shape=jax.ShapeDtypeStruct((blocks, LANES, LANES), jnp.float32),
        scratch_shapes=[pltpu.VMEM(series.shape, jnp.float32)] * 4,
        compiler_params=pltpu.CompilerParams(vmem_limit_bytes=12 << 20),
        cost_estimate=COST,
        name="box",
    )(series, widths)


def pair_kernel(own_ref, other_ref, out_ref):
    blocks = own_ref.shape[0] // 2
    total = own_ref[:blocks] + other_ref[:blocks]
    apart = own_ref[:blocks] - other_ref[:blocks]
    squares = own_ref[blocks:] + other_ref[blocks:] + apart * apart * (0.5 / LANES)
    both = jnp.concatenate([total, squares], 0)
    out_ref[...] = jnp.broadcast_to(both[None], out_ref.shape)


def pair_stage(own, other, peers):
    return pl.pallas_call(
        pair_kernel,
        out_shape=jax.ShapeDtypeStruct((peers, *own.shape), jnp.float32),
        compiler_params=pltpu.CompilerParams(vmem_limit_bytes=8 << 20),
        name="pair",
    )(own, other)


def snr_kernel(samples, period, box_ref, stat_ref, width_ref, out_hbm, done, sems):
    sources, stat_rows, _ = stat_ref.shape
    blocks = stat_rows // 2
    turns = blocks // period
    own = samples // sources
    totals = stat_ref[:, :blocks, :]
    average = jnp.sum(totals, 0) * (1.0 / samples)
    apart = totals * (1.0 / own) - average[None]
    squares = jnp.sum(stat_ref[:, blocks:, :], 0) + own * jnp.sum(apart * apart, 0)
    variance = squares * (1.0 / samples)
    width = jnp.concatenate([width_ref[pl.ds(j, turns, period), :] for j in range(period)], 0)
    width = width.astype(jnp.float32)
    scale = 1.0 / jnp.sqrt(width * (variance + 1e-05))
    level = width * average
    copies = []
    for turn in range(turns):
        for j in range(period):
            row = j * turns + turn
            block = turn * period + j
            value = (box_ref[block] - level[row : row + 1]) * scale[row : row + 1]
            done[block * LANES : (block + 1) * LANES, :] = value.T
        span = slice(turn * period * LANES, (turn + 1) * period * LANES)
        copy = pltpu.make_async_copy(done.at[span, :], out_hbm.at[span, :], sems.at[turn])
        copy.start()
        copies.append(copy)
    for copy in copies:
        copy.wait()


def snr_stage(box, stats, widths, samples, period):
    blocks = widths.shape[0]
    turns = blocks // period
    return pl.pallas_call(
        functools.partial(snr_kernel, samples, period),
        out_shape=jax.ShapeDtypeStruct((blocks * LANES, LANES), jnp.float32),
        out_specs=pl.BlockSpec(memory_space=pltpu.HBM),
        scratch_shapes=[
            pltpu.VMEM((blocks * LANES, LANES), jnp.float32),
            pltpu.SemaphoreType.DMA((turns,)),
        ],
        compiler_params=pltpu.CompilerParams(vmem_limit_bytes=8 << 20),
        name="snr",
    )(box, stats, widths)


def per_device(filterbank, chan_delay, sub_delay, widths):
    samples = filterbank.shape[1]
    groups = chan_delay.shape[0]
    per_group = sub_delay.shape[0] // groups
    chips, cores = lax.axis_size("chip"), lax.axis_size("core")
    widths = widths.reshape(-1, LANES)
    sent = band_stage(filterbank, chan_delay, chips * cores)
    held = lax.all_to_all(sent, ("chip", "core"), split_axis=0, concat_axis=0, tiled=True)
    series, stats = series_stage(held, sub_delay.T, groups)
    other = lax.ppermute(stats, "core", [(0, 1), (1, 0)])
    box = box_stage(series, widths, per_group)
    other, box = lax.optimization_barrier((other, box))
    stats = pair_stage(stats, other, chips)
    stats = lax.all_to_all(stats, "chip", split_axis=0, concat_axis=0, tiled=True)
    return snr_stage(box, stats, widths, samples, pieces_of(per_group)[0])


def solution(mesh):
    beams, devices = mesh.devices.shape
    split = jax.sharding.Mesh(
        mesh.devices.reshape(beams, devices // 2, 2), ("beam", "chip", "core")
    )
    lines = ("chip", "core")
    in_specs = (P(("beam", *lines), None), P(None, lines), P(), P())
    out_specs = P("beam", lines)
    return jax.shard_map(
        per_device, mesh=split, in_specs=in_specs, out_specs=out_specs, check_vma=False
    )
```

```python
import functools
import math

import jax
import jax.numpy as jnp
from jax import lax
from jax.experimental import pallas as pl
from jax.experimental.pallas import tpu as pltpu
from jax.sharding import PartitionSpec as P

SUBCH = 32
DELAY_ONE = 8
DELAY_TWO = 16
WMAX = 16
LANES = 128
HALO = 32
NEAR = 4
FAR = DELAY_TWO // 2
FETCHES = 1
OUT_BLOCKS = 2
PACE = 16
COST = pl.CostEstimate(flops=1 << 28, bytes_accessed=1 << 20, transcendentals=0)


def band_kernel(sub_count, groups, run, fb_hbm, delay_hbm, out_ref, held, delays_ref, carry, tile, sems):
    slabs = out_ref.shape[0]
    channels, samples = fb_hbm.shape
    rows = sub_count * groups
    fetch_delays = pltpu.make_async_copy(delay_hbm, delays_ref, sems.at[0])
    piece = samples // FETCHES
    fetches = [
        pltpu.make_async_copy(
            fb_hbm.at[:, p * piece : (p + 1) * piece],
            held.at[:, p * piece : (p + 1) * piece],
            sems.at[p + 1],
        )
        for p in range(FETCHES)
    ]
    fetch_delays.start()
    for fetch in reversed(fetches):
        fetch.start()
    held[:, samples:] = jnp.zeros((channels, LANES), held.dtype)
    carry[...] = jnp.zeros(carry.shape, carry.dtype)
    out_ref[slabs - 1, rows:, :] = jnp.zeros((rows // 4, LANES), out_ref.dtype)
    fetch_delays.wait()
    delays = delays_ref[...]
    band_of = lax.broadcasted_iota(jnp.int32, delays.shape, 1) // SUBCH
    hot = []
    for far in range(0, DELAY_ONE, NEAR):
        for band in range(sub_count):
            hot.append(
                jnp.concatenate(
                    [
                        jnp.where((delays == far + near) & (band_of == band), 1.0, 0.0)
                        for near in range(NEAR)
                    ],
                    1,
                )
            )
    hot = jnp.concatenate(hot, 0).astype(jnp.bfloat16)
    lane = lax.broadcasted_iota(jnp.int32, (channels, LANES), 1)
    out_lane = lax.broadcasted_iota(jnp.int32, (rows, LANES), 1)
    place = lax.broadcasted_iota(jnp.int32, (4 * LANES, LANES), 0)
    place_out = lax.broadcasted_iota(jnp.int32, (4 * LANES, LANES), 1)
    fold = (place % LANES < HALO) & (place // LANES * HALO + place % LANES == place_out)
    fold = jnp.where(fold, 1.0, 0.0)
    for fetch in fetches:
        fetch.wait()

    pace = math.gcd(run, PACE)

    def turn(i, _):
        first = (slabs // run - 1 - i) * run

        def tile_at(j):
            return held[:, pl.ds(pl.multiple_of((first + j) * LANES, LANES), LANES)]

        def turned_all(j):
            block = tile_at(j)
            return [block] + [pltpu.roll(block, LANES - near, 1) for near in range(1, NEAR)]

        following = [jnp.zeros((channels, LANES), held.dtype)] * NEAR if run == slabs else turned_all(run)
        late = carry[...]
        for pack in range(run // pace - 1, -1, -1):
            sides = [None] * pace
            for side in range(pace - 1, -1, -1):
                here = turned_all(pace * pack + side)
                sides[side] = jnp.concatenate(
                    [here[0]]
                    + [
                        jnp.where(lane < LANES - near, here[near], following[near])
                        for near in range(1, NEAR)
                    ],
                    0,
                )
                following = here
            parts = jnp.dot(hot, jnp.concatenate(sides, 1), preferred_element_type=jnp.float32)
            for side in range(pace - 1, -1, -1):
                part = parts[:, side * LANES : (side + 1) * LANES]
                total = part[:rows]
                fresh = pltpu.roll(part[rows:], LANES - NEAR, 1)
                total = total + jnp.where(out_lane < LANES - NEAR, fresh, late)
                late = fresh
                total = total.astype(jnp.bfloat16)
                slot = pace * pack + side
                out_ref[first + slot, :rows, :] = total
                tile[slot * rows : (slot + 1) * rows, :] = total.astype(jnp.float32)
        ends = jnp.concatenate(
            [tile[pl.ds(q, run * rows // 4, 4), :] for q in range(4)], 1
        )
        ends = jnp.dot(ends, fold, preferred_element_type=jnp.float32).astype(out_ref.dtype)
        for slot in range(run):
            end = ends[slot * rows // 4 : (slot + 1) * rows // 4]
            if slot:
                out_ref[first + slot - 1, rows:, :] = end
            else:
                @pl.when(first > 0)
                def _():
                    out_ref[first - 1, rows:, :] = end
        carry[...] = late
        return 0

    if run == slabs:
        turn(0, 0)
    else:
        lax.fori_loop(0, slabs // run, turn, 0)


def band_stage(filterbank, chan_delay, slabs):
    groups = chan_delay.shape[0]
    channels, samples = filterbank.shape
    rows = channels // SUBCH * groups
    run = math.gcd(slabs, 16)
    return pl.pallas_call(
        functools.partial(band_kernel, channels // SUBCH, groups, run),
        out_shape=jax.ShapeDtypeStruct((slabs, rows + rows // 4, LANES), jnp.bfloat16),
        in_specs=[pl.BlockSpec(memory_space=pltpu.HBM)] * 2,
        scratch_shapes=[
            pltpu.VMEM((channels, samples + LANES), jnp.bfloat16),
            pltpu.VMEM(chan_delay.shape, jnp.int32),
            pltpu.VMEM((rows, LANES), jnp.float32),
            pltpu.VMEM((run * rows, LANES), jnp.float32),
            pltpu.SemaphoreType.DMA((FETCHES + 1,)),
        ],
        compiler_params=pltpu.CompilerParams(vmem_limit_bytes=(8 << 20) + 2 * filterbank.size),
        name="bands",
    )(*(pltpu.with_memory_space_constraint(x, pltpu.HBM) for x in (filterbank, chan_delay)))


def group_lanes(block_rows, group, per_group):
    start = group * per_group
    first, shift = start // LANES, start % LANES
    front = block_rows(first)
    if shift + per_group <= LANES:
        return front
    lane = lax.broadcasted_iota(jnp.int32, front.shape, 1)
    return jnp.where(lane < shift, block_rows(first + 1), front)


def one_hot(delays, first, count):
    return jnp.concatenate([jnp.where(delays == first + e, 1.0, 0.0) for e in range(count)], 0)


def pieces_of(per_group):
    period = per_group // HALO
    starts = [LANES * m // per_group for m in range(period)]
    splits = [per_group * (g + 1) - LANES * m for m, g in enumerate(starts)]
    return period, starts, splits


def series_kernel(whole, per_group, held_ref, delay_ref, series_ref, stat_ref, wide, slid, dense, near, rows_at):
    sources, row_count, _ = held_ref.shape
    groups = series_ref.shape[0]
    bands, trials = delay_ref.shape
    per_source = bands // sources
    rows = per_source * groups
    pitch = row_count + 1
    copies = max(1, LANES // bands)
    span = LANES + WMAX
    base = 8
    for block in range(trials // LANES):
        dense[block] = delay_ref[:, block * LANES : (block + 1) * LANES]

    def ordered(block):
        return jnp.concatenate(
            [dense[block, pl.ds(b, sources, per_source), :] for b in range(per_source)], 0
        )

    for group in range(groups):
        near[group] = group_lanes(ordered, group, per_group)
    for source in range(sources):
        wide[source * pitch : source * pitch + row_count, :] = held_ref[source].astype(jnp.float32)

    def turned(first_row, stride):
        picked = [
            wide[pl.ds(first_row + part * stride, sources, pitch), :] for part in range(per_source)
        ]
        return jnp.concatenate(picked * copies, 0).T

    def store(q, first, block):
        slid[q, base + first : base + first + block.shape[0], :] = block

    def store_slid(q, first, block):
        for copy in range(1, copies):
            low = copy * bands
            top = low + bands
            begin = base + first - copy
            slid[q, begin : begin + block.shape[0], low:top] = block[:, low:top]

    def quad_of(quad, at):
        tails = turned(rows + quad, groups // 4)
        for q in range(4):
            group = quad * 4 + q
            place = at + q
            body = turned(group, groups)
            tail = tails[q * HALO : (q + 1) * HALO]
            store(place, 0, body)
            store(place, LANES, tail)
            store_slid(place, 0, body)
            store_slid(place, LANES, tail)
            both = jnp.zeros((span + FAR, 2 * LANES), jnp.float32)
            step = 2 * copies
            for offset in range(0, FAR, step):
                hot = jnp.concatenate(
                    [one_hot(near[group], far + offset, step) for far in (0, FAR)], 1
                )
                left = jnp.concatenate(
                    [
                        slid[place, base + o : base + o + span + FAR, :]
                        for o in range(offset, offset + step, copies)
                    ],
                    1,
                )
                both = both + jnp.dot(left, hot, preferred_element_type=jnp.float32)
            out = both[:span, :LANES] + both[FAR:, LANES:]
            series_ref[group] = out
            own = out[:LANES]
            total = jnp.sum(own, 0, keepdims=True)
            centred = own - total * (1.0 / LANES)
            rows_at[0, pl.ds(group, 1), :] = total
            rows_at[1, pl.ds(group, 1), :] = jnp.sum(centred * centred, 0, keepdims=True)

    if whole:
        for quad in range(groups // 4):
            quad_of(quad, quad * 4)
    else:

        def turn(quad, _):
            quad_of(quad, 0)
            return 0

        lax.fori_loop(0, groups // 4, turn, 0)

    period, starts, splits = pieces_of(per_group)
    cycle = period + 1
    lane = lax.broadcasted_iota(jnp.int32, (groups // cycle, LANES), 1)
    packed = []
    for stat in range(2):
        moved = [rows_at[stat, pl.ds(q, groups // cycle, cycle), :] for q in range(cycle)]
        for start, split in zip(starts, splits):
            packed.append(jnp.where(lane < split, moved[start], moved[start + 1]))
    stat_ref[...] = jnp.concatenate(packed, 0)


def series_stage(held, delays, groups):
    sources, row_count, _ = held.shape
    bands, trials = delays.shape
    across = max(LANES, bands)
    whole = bands <= LANES
    return pl.pallas_call(
        functools.partial(series_kernel, whole, trials // groups),
        out_shape=(
            jax.ShapeDtypeStruct((groups, LANES + WMAX, LANES), jnp.float32),
            jax.ShapeDtypeStruct((2 * trials // LANES, LANES), jnp.float32),
        ),
        scratch_shapes=[
            pltpu.VMEM((sources * (row_count + 1) + 7, LANES), jnp.float32),
            pltpu.VMEM((groups if whole else 4, LANES + HALO + 8, across), jnp.float32),
            pltpu.VMEM((trials // LANES, bands, LANES), jnp.int32),
            pltpu.VMEM((groups, bands, LANES), jnp.int32),
            pltpu.VMEM((2, groups, LANES), jnp.float32),
        ],
        compiler_params=pltpu.CompilerParams(vmem_limit_bytes=(8 << 20) + (0 if whole else 32 << 20)),
        name="series",
    )(held, delays)


def box_kernel(per_group, series_ref, width_ref, out_ref, pairs, ones, fours, threes):
    groups = series_ref.shape[0]
    period, starts, splits = pieces_of(per_group)
    cycle = period + 1
    lane = lax.broadcasted_iota(jnp.int32, (LANES, LANES), 1)

    def window(ref, group, first, count):
        return ref[group, first : first + count, :]

    def boxes(group):
        width = group_lanes(lambda r: width_ref[r : r + 1, :], group, per_group)
        bits = [width & (1 << e) > 0 for e in range(5)]
        top = LANES + 15
        here = window(series_ref, group, 0, top)
        pairs[group, :top, :] = here + window(series_ref, group, 1, top)
        ones[group, :top, :] = jnp.where(bits[0], here, 0.0)
        top = LANES + 12
        two = window(pairs, group, 0, top)
        fours[group, :top, :] = two + window(pairs, group, 2, top)
        threes[group, :top, :] = jnp.where(
            bits[1], two + window(ones, group, 2, top), window(ones, group, 0, top)
        )
        top = LANES + 8
        four = window(fours, group, 0, top)
        eight = four + window(fours, group, 4, top)
        seven = jnp.where(
            bits[2], four + window(threes, group, 4, top), window(threes, group, 0, top)
        )
        part = jnp.where(bits[3], eight[:LANES] + seven[8:], seven[:LANES])
        return jnp.where(bits[4], eight[:LANES] + eight[8:], part)

    for turn in range(groups // cycle):
        moved = [boxes(turn * cycle + q) for q in range(cycle)]
        for j, (start, split) in enumerate(zip(starts, splits)):
            out_ref[turn * period + j] = jnp.where(lane < split, moved[start], moved[start + 1])


def box_stage(series, widths, per_group):
    blocks = widths.shape[0]
    return pl.pallas_call(
        functools.partial(box_kernel, per_group),
        out_shape=jax.ShapeDtypeStruct((blocks, LANES, LANES), jnp.float32),
        scratch_shapes=[pltpu.VMEM(series.shape, jnp.float32)] * 4,
        compiler_params=pltpu.CompilerParams(vmem_limit_bytes=12 << 20),
        cost_estimate=COST,
        name="box",
    )(series, widths)


def pair_kernel(own_ref, other_ref, out_ref):
    blocks = own_ref.shape[0] // 2
    total = own_ref[:blocks] + other_ref[:blocks]
    apart = own_ref[:blocks] - other_ref[:blocks]
    squares = own_ref[blocks:] + other_ref[blocks:] + apart * apart * (0.5 / LANES)
    both = jnp.concatenate([total, squares], 0)
    out_ref[...] = jnp.broadcast_to(both[None], out_ref.shape)


def pair_stage(own, other, peers):
    return pl.pallas_call(
        pair_kernel,
        out_shape=jax.ShapeDtypeStruct((peers, *own.shape), jnp.float32),
        compiler_params=pltpu.CompilerParams(vmem_limit_bytes=8 << 20),
        name="pair",
    )(own, other)


def snr_kernel(samples, period, box_ref, stat_ref, width_ref, out_hbm, done, sems):
    sources, stat_rows, _ = stat_ref.shape
    blocks = stat_rows // 2
    turns = blocks // period
    own = samples // sources
    totals = stat_ref[:, :blocks, :]
    average = jnp.sum(totals, 0) * (1.0 / samples)
    apart = totals * (1.0 / own) - average[None]
    squares = jnp.sum(stat_ref[:, blocks:, :], 0) + own * jnp.sum(apart * apart, 0)
    variance = squares * (1.0 / samples)
    width = jnp.concatenate([width_ref[pl.ds(j, turns, period), :] for j in range(period)], 0)
    width = width.astype(jnp.float32)
    scale = lax.rsqrt(width * (variance + 1e-05))
    level = width * average
    copies = []
    for block in range(blocks):
        row = block % period * turns + block // period
        span = slice(block * LANES, (block + 1) * LANES)
        value = (box_ref[block] - level[row : row + 1]) * scale[row : row + 1]
        done[span, :] = value.T
        if (block + 1) % OUT_BLOCKS == 0:
            span = slice((block + 1 - OUT_BLOCKS) * LANES, (block + 1) * LANES)
            copy = pltpu.make_async_copy(
                done.at[span, :], out_hbm.at[span, :], sems.at[block // OUT_BLOCKS]
            )
            copy.start()
            copies.append(copy)
    for copy in copies:
        copy.wait()


def snr_stage(box, stats, widths, samples, period):
    blocks = widths.shape[0]
    return pl.pallas_call(
        functools.partial(snr_kernel, samples, period),
        out_shape=jax.ShapeDtypeStruct((blocks * LANES, LANES), jnp.float32),
        out_specs=pl.BlockSpec(memory_space=pltpu.HBM),
        scratch_shapes=[
            pltpu.VMEM((blocks * LANES, LANES), jnp.float32),
            pltpu.SemaphoreType.DMA((blocks // OUT_BLOCKS,)),
        ],
        compiler_params=pltpu.CompilerParams(vmem_limit_bytes=8 << 20),
        name="snr",
    )(box, stats, widths)


def per_device(filterbank, chan_delay, sub_delay, widths):
    samples = filterbank.shape[1]
    groups = chan_delay.shape[0]
    per_group = sub_delay.shape[0] // groups
    chips, cores = lax.axis_size("chip"), lax.axis_size("core")
    widths = widths.reshape(-1, LANES)
    sent = band_stage(filterbank, chan_delay, chips * cores)
    held = lax.all_to_all(sent, ("chip", "core"), split_axis=0, concat_axis=0, tiled=True)
    series, stats = series_stage(held, sub_delay.T, groups)
    other = lax.ppermute(stats, "core", [(0, 1), (1, 0)])
    box = box_stage(series, widths, per_group)
    other, box = lax.optimization_barrier((other, box))
    stats = pair_stage(stats, other, chips)
    stats = lax.all_to_all(stats, "chip", split_axis=0, concat_axis=0, tiled=True)
    return snr_stage(box, stats, widths, samples, pieces_of(per_group)[0])


def solution(mesh):
    beams, devices = mesh.devices.shape
    split = jax.sharding.Mesh(
        mesh.devices.reshape(beams, devices // 2, 2), ("beam", "chip", "core")
    )
    lines = ("chip", "core")
    in_specs = (P(("beam", *lines), None), P(None, lines), P(), P())
    out_specs = P("beam", lines)
    return jax.shard_map(
        per_device, mesh=split, in_specs=in_specs, out_specs=out_specs, check_vma=False
    )
```

```python
import functools
import math

import jax
import jax.numpy as jnp
from jax import lax
from jax.experimental import pallas as pl
from jax.experimental.pallas import tpu as pltpu
from jax.sharding import PartitionSpec as P

SUBCH = 32
DELAY_ONE = 8
DELAY_TWO = 16
WMAX = 16
LANES = 128
HALO = 32
NEAR = 4
FAR = DELAY_TWO // 2
FETCHES = 1
OUT_BLOCKS = 2
PACE = 16
COST = pl.CostEstimate(flops=1 << 28, bytes_accessed=1 << 20, transcendentals=0)


def band_kernel(sub_count, groups, run, fb_hbm, delay_hbm, out_ref, held, delays_ref, carry, tile, sems):
    slabs = out_ref.shape[0]
    channels, samples = fb_hbm.shape
    rows = sub_count * groups
    fetch_delays = pltpu.make_async_copy(delay_hbm, delays_ref, sems.at[0])
    piece = samples // FETCHES
    fetches = [
        pltpu.make_async_copy(
            fb_hbm.at[:, p * piece : (p + 1) * piece],
            held.at[:, p * piece : (p + 1) * piece],
            sems.at[p + 1],
        )
        for p in range(FETCHES)
    ]
    fetch_delays.start()
    for fetch in reversed(fetches):
        fetch.start()
    held[:, samples:] = jnp.zeros((channels, LANES), held.dtype)
    carry[...] = jnp.zeros(carry.shape, carry.dtype)
    part = rows // 2
    for core in range(2):
        out_ref[slabs - 2 + core, rows:, :] = jnp.zeros((rows // 8, LANES), out_ref.dtype)
    fetch_delays.wait()
    delays = delays_ref[...]
    band_of = lax.broadcasted_iota(jnp.int32, delays.shape, 1) // SUBCH
    hot = []
    for far in range(0, DELAY_ONE, NEAR):
        for core in range(2):
            wanted = delays[core * groups // 2 : (core + 1) * groups // 2]
            for band in range(sub_count):
                mine = band_of[: groups // 2] == band
                hot.append(
                    jnp.concatenate(
                        [
                            jnp.where((wanted == far + near) & mine, 1.0, 0.0)
                            for near in range(NEAR)
                        ],
                        1,
                    )
                )
    hot = jnp.concatenate(hot, 0).astype(jnp.bfloat16)
    lane = lax.broadcasted_iota(jnp.int32, (channels, LANES), 1)
    out_lane = lax.broadcasted_iota(jnp.int32, (rows, LANES), 1)
    place = lax.broadcasted_iota(jnp.int32, (4 * LANES, LANES), 0)
    place_out = lax.broadcasted_iota(jnp.int32, (4 * LANES, LANES), 1)
    fold = (place % LANES < HALO) & (place // LANES * HALO + place % LANES == place_out)
    fold = jnp.where(fold, 1.0, 0.0)
    for fetch in fetches:
        fetch.wait()

    pace = math.gcd(run, PACE)

    def turn(i, _):
        first = (slabs // run - 1 - i) * run

        def tile_at(j):
            return held[:, pl.ds(pl.multiple_of((first + j) * LANES, LANES), LANES)]

        def turned_all(j):
            block = tile_at(j)
            return [block] + [pltpu.roll(block, LANES - near, 1) for near in range(1, NEAR)]

        following = [jnp.zeros((channels, LANES), held.dtype)] * NEAR if run == slabs else turned_all(run)
        late = carry[...]
        for pack in range(run // pace - 1, -1, -1):
            sides = [None] * pace
            for side in range(pace - 1, -1, -1):
                here = turned_all(pace * pack + side)
                sides[side] = jnp.concatenate(
                    [here[0]]
                    + [
                        jnp.where(lane < LANES - near, here[near], following[near])
                        for near in range(1, NEAR)
                    ],
                    0,
                )
                following = here
            parts = jnp.dot(hot, jnp.concatenate(sides, 1), preferred_element_type=jnp.float32)
            for side in range(pace - 1, -1, -1):
                here = parts[:, side * LANES : (side + 1) * LANES]
                total = here[:rows]
                fresh = pltpu.roll(here[rows:], LANES - NEAR, 1)
                total = total + jnp.where(out_lane < LANES - NEAR, fresh, late)
                late = fresh
                total = total.astype(jnp.bfloat16)
                slot = pace * pack + side
                lead = first + slot // 2 * 2
                low = slot % 2 * part
                for core in range(2):
                    out_ref[lead + core, low : low + part, :] = total[core * part : (core + 1) * part]
                if slot % 2 == 0:
                    at = slot // 2 * rows
                    tile[at : at + rows, :] = total.astype(jnp.float32)
        ends = jnp.concatenate(
            [tile[pl.ds(q, run * rows // 8, 4), :] for q in range(4)], 1
        )
        ends = jnp.dot(ends, fold, preferred_element_type=jnp.float32)
        for pair in range(run // 2):
            for core in range(2):
                at = (2 * pair + core) * rows // 8
                end = ends[at : at + rows // 8].astype(out_ref.dtype)
                if pair:
                    out_ref[first + 2 * pair - 2 + core, rows:, :] = end
                else:
                    @pl.when(first > 0)
                    def _():
                        out_ref[first - 2 + core, rows:, :] = end
        carry[...] = late
        return 0

    if run == slabs:
        turn(0, 0)
    else:
        lax.fori_loop(0, slabs // run, turn, 0)


def band_stage(filterbank, chan_delay, slabs):
    groups = chan_delay.shape[0]
    channels, samples = filterbank.shape
    rows = channels // SUBCH * groups
    run = math.gcd(slabs, 16)
    return pl.pallas_call(
        functools.partial(band_kernel, channels // SUBCH, groups, run),
        out_shape=jax.ShapeDtypeStruct((slabs, rows + rows // 8, LANES), jnp.bfloat16),
        in_specs=[pl.BlockSpec(memory_space=pltpu.HBM)] * 2,
        scratch_shapes=[
            pltpu.VMEM((channels, samples + LANES), jnp.bfloat16),
            pltpu.VMEM(chan_delay.shape, jnp.int32),
            pltpu.VMEM((rows, LANES), jnp.float32),
            pltpu.VMEM((run * rows // 2, LANES), jnp.float32),
            pltpu.SemaphoreType.DMA((FETCHES + 1,)),
        ],
        compiler_params=pltpu.CompilerParams(vmem_limit_bytes=(8 << 20) + 2 * filterbank.size),
        name="bands",
    )(*(pltpu.with_memory_space_constraint(x, pltpu.HBM) for x in (filterbank, chan_delay)))


def group_lanes(block_rows, group, per_group):
    start = group * per_group
    first, shift = start // LANES, start % LANES
    front = block_rows(first)
    if shift + per_group <= LANES:
        return front
    lane = lax.broadcasted_iota(jnp.int32, front.shape, 1)
    return jnp.where(lane < shift, block_rows(first + 1), front)


def one_hot(delays, first, count):
    return jnp.concatenate([jnp.where(delays == first + e, 1.0, 0.0) for e in range(count)], 0)


def pieces_of(per_group):
    period = per_group // HALO
    starts = [LANES * m // per_group for m in range(period)]
    splits = [per_group * (g + 1) - LANES * m for m, g in enumerate(starts)]
    return period, starts, splits


def series_kernel(whole, per_group, held_ref, delay_ref, series_ref, stat_ref, wide, slid, dense, near, rows_at):
    sources, row_count, _ = held_ref.shape
    groups = series_ref.shape[0]
    bands, trials = delay_ref.shape
    per_source = bands // sources
    part = per_source * groups
    blocks = trials // 2 // LANES
    pitch = row_count + 1
    copies = max(1, LANES // bands)
    slab = 2 * LANES
    span = slab + WMAX
    base = 8
    lead = lax.axis_index("core") * blocks
    for block in range(blocks):
        at = pl.multiple_of((lead + block) * LANES, LANES)
        dense[block] = delay_ref[:, pl.ds(at, LANES)]

    def ordered(block):
        return jnp.concatenate(
            [dense[block, pl.ds(b, sources, per_source), :] for b in range(per_source)], 0
        )

    for group in range(groups):
        near[group] = group_lanes(ordered, group, per_group)
    for source in range(sources):
        wide[source * pitch : source * pitch + row_count, :] = held_ref[source].astype(jnp.float32)

    def turned(first_row, stride):
        picked = [
            wide[pl.ds(first_row + b * stride, sources, pitch), :] for b in range(per_source)
        ]
        return jnp.concatenate(picked * copies, 0).T

    def store(q, first, block):
        slid[q, base + first : base + first + block.shape[0], :] = block

    def store_slid(q, first, block):
        for copy in range(1, copies):
            low = copy * bands
            top = low + bands
            begin = base + first - copy
            slid[q, begin : begin + block.shape[0], low:top] = block[:, low:top]

    def quad_of(quad, at):
        tails = turned(2 * part + quad, groups // 4)
        for q in range(4):
            group = quad * 4 + q
            place = at + q
            pieces = [turned(side * part + group, groups) for side in range(2)]
            pieces.append(tails[q * HALO : (q + 1) * HALO])
            for side, piece in enumerate(pieces):
                store(place, side * LANES, piece)
            for side, piece in enumerate(pieces):
                store_slid(place, side * LANES, piece)
            both = jnp.zeros((span + FAR, 2 * LANES), jnp.float32)
            step = 2 * copies
            for offset in range(0, FAR, step):
                hot = jnp.concatenate(
                    [one_hot(near[group], far + offset, step) for far in (0, FAR)], 1
                )
                left = jnp.concatenate(
                    [
                        slid[place, base + o : base + o + span + FAR, :]
                        for o in range(offset, offset + step, copies)
                    ],
                    1,
                )
                both = both + jnp.dot(left, hot, preferred_element_type=jnp.float32)
            out = both[:span, :LANES] + both[FAR:, LANES:]
            series_ref[group] = out
            own = out[:slab]
            total = jnp.sum(own, 0, keepdims=True)
            centred = own - total * (1.0 / slab)
            rows_at[0, pl.ds(group, 1), :] = total
            rows_at[1, pl.ds(group, 1), :] = jnp.sum(centred * centred, 0, keepdims=True)

    if whole:
        for quad in range(groups // 4):
            quad_of(quad, quad * 4)
    else:

        def turn(quad, _):
            quad_of(quad, 0)
            return 0

        lax.fori_loop(0, groups // 4, turn, 0)

    period, starts, splits = pieces_of(per_group)
    cycle = period + 1
    lane = lax.broadcasted_iota(jnp.int32, (groups // cycle, LANES), 1)
    packed = []
    for stat in range(2):
        moved = [rows_at[stat, pl.ds(q, groups // cycle, cycle), :] for q in range(cycle)]
        for start, split in zip(starts, splits):
            packed.append(jnp.where(lane < split, moved[start], moved[start + 1]))
    stat_ref[...] = jnp.concatenate(packed, 0)


def series_stage(held, delays, groups):
    sources, row_count, _ = held.shape
    bands, trials = delays.shape
    across = max(LANES, bands)
    whole = bands <= LANES
    half = groups // 2
    return pl.pallas_call(
        functools.partial(series_kernel, whole, trials // groups),
        out_shape=(
            jax.ShapeDtypeStruct((half, 2 * LANES + WMAX, LANES), jnp.float32),
            jax.ShapeDtypeStruct((trials // LANES, LANES), jnp.float32),
        ),
        scratch_shapes=[
            pltpu.VMEM((sources * (row_count + 1) + 7, LANES), jnp.float32),
            pltpu.VMEM((half if whole else 4, 2 * LANES + HALO + 8, across), jnp.float32),
            pltpu.VMEM((trials // 2 // LANES, bands, LANES), jnp.int32),
            pltpu.VMEM((half, bands, LANES), jnp.int32),
            pltpu.VMEM((2, half, LANES), jnp.float32),
        ],
        compiler_params=pltpu.CompilerParams(vmem_limit_bytes=(8 << 20) + (0 if whole else 32 << 20)),
        name="series",
    )(held, delays)


def box_kernel(per_group, series_ref, width_ref, keep_ref, send_ref, pairs, ones, fours, threes):
    groups = series_ref.shape[0]
    slab = 2 * LANES
    period, starts, splits = pieces_of(per_group)
    cycle = period + 1
    blocks = keep_ref.shape[0]
    core = lax.axis_index("core")
    lane = lax.broadcasted_iota(jnp.int32, (LANES, LANES), 1)

    def window(ref, group, first, count):
        return ref[group, first : first + count, :]

    def boxes(group):
        width = group_lanes(
            lambda r: width_ref[pl.ds(core * blocks + r, 1), :], group, per_group
        )
        bits = [width & (1 << e) > 0 for e in range(5)]
        top = slab + 15
        here = window(series_ref, group, 0, top)
        pairs[group, :top, :] = here + window(series_ref, group, 1, top)
        ones[group, :top, :] = jnp.where(bits[0], here, 0.0)
        top = slab + 12
        two = window(pairs, group, 0, top)
        fours[group, :top, :] = two + window(pairs, group, 2, top)
        threes[group, :top, :] = jnp.where(
            bits[1], two + window(ones, group, 2, top), window(ones, group, 0, top)
        )
        sides = []
        for side in range(0, slab, LANES):
            top = LANES + 8
            four = window(fours, group, side, top)
            eight = four + window(fours, group, side + 4, top)
            seven = jnp.where(
                bits[2],
                four + window(threes, group, side + 4, top),
                window(threes, group, side, top),
            )
            some = jnp.where(bits[3], eight[:LANES] + seven[8:], seven[:LANES])
            sides.append(jnp.where(bits[4], eight[:LANES] + eight[8:], some))
        return sides

    for turn in range(groups // cycle):
        moved = [boxes(turn * cycle + q) for q in range(cycle)]
        for j, (start, split) in enumerate(zip(starts, splits)):
            early, late = (
                jnp.where(lane < split, moved[start][side], moved[start + 1][side])
                for side in range(2)
            )
            keep_ref[turn * period + j] = jnp.where(core == 0, early, late)
            send_ref[turn * period + j] = jnp.where(core == 0, late, early)


def box_stage(series, widths, per_group):
    blocks = widths.shape[0] // 2
    return pl.pallas_call(
        functools.partial(box_kernel, per_group),
        out_shape=[jax.ShapeDtypeStruct((blocks, LANES, LANES), jnp.float32)] * 2,
        scratch_shapes=[pltpu.VMEM(series.shape, jnp.float32)] * 4,
        compiler_params=pltpu.CompilerParams(vmem_limit_bytes=12 << 20),
        cost_estimate=COST,
        name="box",
    )(series, widths)


def pair_kernel(own_ref, other_ref, out_ref):
    half = own_ref.shape[0] // 2
    own, other = own_ref[...], other_ref[...]
    first = lax.axis_index("core") == 0
    low = jnp.where(first, own, other)
    high = jnp.where(first, other, own)
    both = jnp.concatenate([low[:half], high[:half], low[half:], high[half:]], 0)
    out_ref[...] = jnp.broadcast_to(both[None], out_ref.shape)


def pair_stage(own, other, peers):
    return pl.pallas_call(
        pair_kernel,
        out_shape=jax.ShapeDtypeStruct((peers, 2 * own.shape[0], LANES), jnp.float32),
        compiler_params=pltpu.CompilerParams(vmem_limit_bytes=8 << 20),
        name="pair",
    )(own, other)


def snr_kernel(samples, period, keep_ref, came_ref, stat_ref, width_ref, out_hbm, done, levels, sems):
    sources, stat_rows, _ = stat_ref.shape
    blocks = stat_rows // 2
    half = blocks // 2
    turns = half // period
    own = samples // sources
    totals = stat_ref[:, :blocks, :]
    average = jnp.sum(totals, 0) * (1.0 / samples)
    apart = totals * (1.0 / own) - average[None]
    squares = jnp.sum(stat_ref[:, blocks:, :], 0) + own * jnp.sum(apart * apart, 0)
    variance = squares * (1.0 / samples)
    width = jnp.concatenate(
        [width_ref[pl.ds(c * half + j, turns, period), :] for c in range(2) for j in range(period)], 0
    )
    width = width.astype(jnp.float32)
    levels[0] = width * average
    levels[1] = lax.rsqrt(width * (variance + 1e-05))
    core = lax.axis_index("core")
    copies = []
    for order, (box_ref, place) in enumerate(((keep_ref, core), (came_ref, 1 - core))):
        for block in range(half):
            row = place * half + block % period * turns + block // period
            at = order * half + block
            level = levels[0, pl.ds(row, 1), :]
            scale = levels[1, pl.ds(row, 1), :]
            done[at * LANES : (at + 1) * LANES, :] = ((box_ref[block] - level) * scale).T
            if (block + 1) % OUT_BLOCKS == 0:
                size = OUT_BLOCKS * LANES
                target = pl.multiple_of((place * half + block + 1 - OUT_BLOCKS) * LANES, LANES)
                copy = pltpu.make_async_copy(
                    done.at[(at + 1) * LANES - size : (at + 1) * LANES, :],
                    out_hbm.at[pl.ds(target, size), :],
                    sems.at[at // OUT_BLOCKS],
                )
                copy.start()
                copies.append(copy)
    for copy in copies:
        copy.wait()


def snr_stage(keep, came, stats, widths, samples, period):
    blocks = widths.shape[0]
    return pl.pallas_call(
        functools.partial(snr_kernel, samples, period),
        out_shape=jax.ShapeDtypeStruct((blocks * LANES, LANES), jnp.float32),
        out_specs=pl.BlockSpec(memory_space=pltpu.HBM),
        scratch_shapes=[
            pltpu.VMEM((blocks * LANES, LANES), jnp.float32),
            pltpu.VMEM((2, blocks, LANES), jnp.float32),
            pltpu.SemaphoreType.DMA((blocks // OUT_BLOCKS,)),
        ],
        compiler_params=pltpu.CompilerParams(vmem_limit_bytes=8 << 20),
        name="snr",
    )(keep, came, stats, widths)


def per_device(filterbank, chan_delay, sub_delay, widths):
    samples = filterbank.shape[1]
    groups = chan_delay.shape[0]
    per_group = sub_delay.shape[0] // groups
    chips, cores = lax.axis_size("chip"), lax.axis_size("core")
    widths = widths.reshape(-1, LANES)
    sent = band_stage(filterbank, chan_delay, chips * cores)
    held = lax.all_to_all(sent, ("chip", "core"), split_axis=0, concat_axis=0, tiled=True)
    series, stats = series_stage(held, sub_delay.T, groups)
    swap = [(0, 1), (1, 0)]
    other = lax.ppermute(stats, "core", swap)
    keep, send = box_stage(series, widths, per_group)
    other, send = lax.optimization_barrier((other, send))
    came = lax.ppermute(send, "core", swap)
    stats = pair_stage(stats, other, chips)
    stats = lax.all_to_all(stats, "chip", split_axis=0, concat_axis=0, tiled=True)
    return snr_stage(keep, came, stats, widths, samples, pieces_of(per_group)[0])


def solution(mesh):
    beams, devices = mesh.devices.shape
    split = jax.sharding.Mesh(
        mesh.devices.reshape(beams, devices // 2, 2), ("beam", "chip", "core")
    )
    lines = ("chip", "core")
    in_specs = (P(("beam", *lines), None), P(None, lines), P(), P())
    out_specs = P("beam", lines)
    return jax.shard_map(
        per_device, mesh=split, in_specs=in_specs, out_specs=out_specs, check_vma=False
    )
```

```python
import functools
import math

import jax
import jax.numpy as jnp
from jax import lax
from jax.experimental import pallas as pl
from jax.experimental.pallas import tpu as pltpu
from jax.sharding import PartitionSpec as P

SUBCH = 32
DELAY_ONE = 8
DELAY_TWO = 16
WMAX = 16
LANES = 128
HALO = 32
NEAR = 2
FAR = DELAY_TWO // 2
FETCHES = 1
OUT_BLOCKS = 2
PACE = 4
COST = pl.CostEstimate(flops=1 << 28, bytes_accessed=1 << 20, transcendentals=0)


def band_kernel(sub_count, groups, run, fb_hbm, delay_hbm, out_ref, held, delays_ref, carry, tile, sems):
    slabs = out_ref.shape[0]
    channels, samples = fb_hbm.shape
    rows = sub_count * groups
    fetch_delays = pltpu.make_async_copy(delay_hbm, delays_ref, sems.at[0])
    piece = samples // FETCHES
    fetches = [
        pltpu.make_async_copy(
            fb_hbm.at[:, p * piece : (p + 1) * piece],
            held.at[:, p * piece : (p + 1) * piece],
            sems.at[p + 1],
        )
        for p in range(FETCHES)
    ]
    fetch_delays.start()
    for fetch in reversed(fetches):
        fetch.start()
    held[:, samples:] = jnp.zeros((channels, LANES), held.dtype)
    carry[...] = jnp.zeros(carry.shape, carry.dtype)
    part = rows // 2
    for core in range(2):
        out_ref[slabs - 2 + core, rows:, :] = jnp.zeros((rows // 8, LANES), out_ref.dtype)
    fetch_delays.wait()
    delays = delays_ref[...]
    band_of = lax.broadcasted_iota(jnp.int32, delays.shape, 1) // SUBCH
    hot = []
    for far in range(0, DELAY_ONE, NEAR):
        for core in range(2):
            wanted = delays[core * groups // 2 : (core + 1) * groups // 2]
            for band in range(sub_count):
                mine = band_of[: groups // 2] == band
                hot.append(
                    jnp.concatenate(
                        [
                            jnp.where((wanted == far + near) & mine, 1.0, 0.0)
                            for near in range(NEAR)
                        ],
                        1,
                    )
                )
    hot = jnp.concatenate(hot, 0).astype(jnp.bfloat16)
    lane = lax.broadcasted_iota(jnp.int32, (channels, LANES), 1)
    out_lane = lax.broadcasted_iota(jnp.int32, (rows, LANES), 1)
    place = lax.broadcasted_iota(jnp.int32, (4 * LANES, LANES), 0)
    place_out = lax.broadcasted_iota(jnp.int32, (4 * LANES, LANES), 1)
    fold = (place % LANES < HALO) & (place // LANES * HALO + place % LANES == place_out)
    fold = jnp.where(fold, 1.0, 0.0)
    for fetch in fetches:
        fetch.wait()

    pace = math.gcd(run, PACE)

    def turn(i, _):
        first = (slabs // run - 1 - i) * run

        def tile_at(j):
            return held[:, pl.ds(pl.multiple_of((first + j) * LANES, LANES), LANES)]

        def turned_all(j):
            block = tile_at(j)
            return [block] + [pltpu.roll(block, LANES - near, 1) for near in range(1, NEAR)]

        following = [jnp.zeros((channels, LANES), held.dtype)] * NEAR if run == slabs else turned_all(run)
        late = [carry[far] for far in range(DELAY_ONE // NEAR - 1)]
        for pack in range(run // pace - 1, -1, -1):
            sides = [None] * pace
            for side in range(pace - 1, -1, -1):
                here = turned_all(pace * pack + side)
                sides[side] = jnp.concatenate(
                    [here[0]]
                    + [
                        jnp.where(lane < LANES - near, here[near], following[near])
                        for near in range(1, NEAR)
                    ],
                    0,
                )
                following = here
            parts = jnp.dot(hot, jnp.concatenate(sides, 1), preferred_element_type=jnp.float32)
            for side in range(pace - 1, -1, -1):
                here = parts[:, side * LANES : (side + 1) * LANES]
                total = here[:rows]
                for far in range(1, DELAY_ONE // NEAR):
                    keep = LANES - far * NEAR
                    fresh = pltpu.roll(here[far * rows : (far + 1) * rows], keep, 1)
                    total = total + jnp.where(out_lane < keep, fresh, late[far - 1])
                    late[far - 1] = fresh
                total = total.astype(jnp.bfloat16)
                slot = pace * pack + side
                lead = first + slot // 2 * 2
                low = slot % 2 * part
                for core in range(2):
                    out_ref[lead + core, low : low + part, :] = total[core * part : (core + 1) * part]
                if slot % 2 == 0:
                    at = slot // 2 * rows
                    tile[at : at + rows, :] = total.astype(jnp.float32)
        ends = jnp.concatenate(
            [tile[pl.ds(q, run * rows // 8, 4), :] for q in range(4)], 1
        )
        ends = jnp.dot(ends, fold, preferred_element_type=jnp.float32)
        for pair in range(run // 2):
            for core in range(2):
                at = (2 * pair + core) * rows // 8
                end = ends[at : at + rows // 8].astype(out_ref.dtype)
                if pair:
                    out_ref[first + 2 * pair - 2 + core, rows:, :] = end
                else:
                    @pl.when(first > 0)
                    def _():
                        out_ref[first - 2 + core, rows:, :] = end
        for far, block in enumerate(late):
            carry[far] = block
        return 0

    if run == slabs:
        turn(0, 0)
    else:
        lax.fori_loop(0, slabs // run, turn, 0)


def band_stage(filterbank, chan_delay, slabs):
    groups = chan_delay.shape[0]
    channels, samples = filterbank.shape
    rows = channels // SUBCH * groups
    run = math.gcd(slabs, 16)
    return pl.pallas_call(
        functools.partial(band_kernel, channels // SUBCH, groups, run),
        out_shape=jax.ShapeDtypeStruct((slabs, rows + rows // 8, LANES), jnp.bfloat16),
        in_specs=[pl.BlockSpec(memory_space=pltpu.HBM)] * 2,
        scratch_shapes=[
            pltpu.VMEM((channels, samples + LANES), jnp.bfloat16),
            pltpu.VMEM(chan_delay.shape, jnp.int32),
            pltpu.VMEM((DELAY_ONE // NEAR - 1, rows, LANES), jnp.float32),
            pltpu.VMEM((run * rows // 2, LANES), jnp.float32),
            pltpu.SemaphoreType.DMA((FETCHES + 1,)),
        ],
        compiler_params=pltpu.CompilerParams(vmem_limit_bytes=(8 << 20) + 2 * filterbank.size),
        name="bands",
    )(*(pltpu.with_memory_space_constraint(x, pltpu.HBM) for x in (filterbank, chan_delay)))


def group_lanes(block_rows, group, per_group):
    start = group * per_group
    first, shift = start // LANES, start % LANES
    front = block_rows(first)
    if shift + per_group <= LANES:
        return front
    lane = lax.broadcasted_iota(jnp.int32, front.shape, 1)
    return jnp.where(lane < shift, block_rows(first + 1), front)


def one_hot(delays, first, count):
    return jnp.concatenate([jnp.where(delays == first + e, 1.0, 0.0) for e in range(count)], 0)


def pieces_of(per_group):
    period = per_group // HALO
    starts = [LANES * m // per_group for m in range(period)]
    splits = [per_group * (g + 1) - LANES * m for m, g in enumerate(starts)]
    return period, starts, splits


def series_kernel(whole, per_group, held_ref, delay_ref, series_ref, stat_ref, wide, slid, dense, near, rows_at):
    sources, row_count, _ = held_ref.shape
    groups = series_ref.shape[0]
    bands, trials = delay_ref.shape
    per_source = bands // sources
    part = per_source * groups
    blocks = trials // 2 // LANES
    pitch = row_count + 1
    copies = max(1, LANES // bands)
    slab = 2 * LANES
    span = slab + WMAX
    base = 8
    lead = lax.axis_index("core") * blocks
    for block in range(blocks):
        at = pl.multiple_of((lead + block) * LANES, LANES)
        dense[block] = delay_ref[:, pl.ds(at, LANES)]

    def ordered(block):
        return jnp.concatenate(
            [dense[block, pl.ds(b, sources, per_source), :] for b in range(per_source)], 0
        )

    for group in range(groups):
        near[group] = group_lanes(ordered, group, per_group)
    for source in range(sources):
        wide[source * pitch : source * pitch + row_count, :] = held_ref[source].astype(jnp.float32)

    def turned(first_row, stride):
        picked = [
            wide[pl.ds(first_row + b * stride, sources, pitch), :] for b in range(per_source)
        ]
        return jnp.concatenate(picked * copies, 0).T

    def store(q, first, block):
        slid[q, base + first : base + first + block.shape[0], :] = block

    def store_slid(q, first, block):
        for copy in range(1, copies):
            low = copy * bands
            top = low + bands
            begin = base + first - copy
            slid[q, begin : begin + block.shape[0], low:top] = block[:, low:top]

    def quad_of(quad, at):
        tails = turned(2 * part + quad, groups // 4)
        for q in range(4):
            group = quad * 4 + q
            place = at + q
            pieces = [turned(side * part + group, groups) for side in range(2)]
            pieces.append(tails[q * HALO : (q + 1) * HALO])
            for side, piece in enumerate(pieces):
                store(place, side * LANES, piece)
            for side, piece in enumerate(pieces):
                store_slid(place, side * LANES, piece)
            both = jnp.zeros((span + FAR, 2 * LANES), jnp.float32)
            step = 2 * copies
            for offset in range(0, FAR, step):
                hot = jnp.concatenate(
                    [one_hot(near[group], far + offset, step) for far in (0, FAR)], 1
                )
                left = jnp.concatenate(
                    [
                        slid[place, base + o : base + o + span + FAR, :]
                        for o in range(offset, offset + step, copies)
                    ],
                    1,
                )
                both = both + jnp.dot(left, hot, preferred_element_type=jnp.float32)
            out = both[:span, :LANES] + both[FAR:, LANES:]
            series_ref[group] = out
            own = out[:slab]
            total = jnp.sum(own, 0, keepdims=True)
            centred = own - total * (1.0 / slab)
            rows_at[0, pl.ds(group, 1), :] = total
            rows_at[1, pl.ds(group, 1), :] = jnp.sum(centred * centred, 0, keepdims=True)

    if whole:
        for quad in range(groups // 4):
            quad_of(quad, quad * 4)
    else:

        def turn(quad, _):
            quad_of(quad, 0)
            return 0

        lax.fori_loop(0, groups // 4, turn, 0)

    period, starts, splits = pieces_of(per_group)
    cycle = period + 1
    lane = lax.broadcasted_iota(jnp.int32, (groups // cycle, LANES), 1)
    packed = []
    for stat in range(2):
        moved = [rows_at[stat, pl.ds(q, groups // cycle, cycle), :] for q in range(cycle)]
        for start, split in zip(starts, splits):
            packed.append(jnp.where(lane < split, moved[start], moved[start + 1]))
    stat_ref[...] = jnp.concatenate(packed, 0)


def series_stage(held, delays, groups):
    sources, row_count, _ = held.shape
    bands, trials = delays.shape
    across = max(LANES, bands)
    whole = bands <= LANES
    half = groups // 2
    return pl.pallas_call(
        functools.partial(series_kernel, whole, trials // groups),
        out_shape=(
            jax.ShapeDtypeStruct((half, 2 * LANES + WMAX, LANES), jnp.float32),
            jax.ShapeDtypeStruct((trials // LANES, LANES), jnp.float32),
        ),
        scratch_shapes=[
            pltpu.VMEM((sources * (row_count + 1) + 7, LANES), jnp.float32),
            pltpu.VMEM((half if whole else 4, 2 * LANES + HALO + 8, across), jnp.float32),
            pltpu.VMEM((trials // 2 // LANES, bands, LANES), jnp.int32),
            pltpu.VMEM((half, bands, LANES), jnp.int32),
            pltpu.VMEM((2, half, LANES), jnp.float32),
        ],
        compiler_params=pltpu.CompilerParams(
            vmem_limit_bytes=(8 << 20) + (0 if whole else 32 << 20),
        ),
        name="series",
    )(held, delays)


def box_kernel(per_group, series_ref, width_ref, keep_ref, send_ref, pairs, ones, fours, threes):
    groups = series_ref.shape[0]
    slab = 2 * LANES
    period, starts, splits = pieces_of(per_group)
    cycle = period + 1
    blocks = keep_ref.shape[0]
    core = lax.axis_index("core")
    lane = lax.broadcasted_iota(jnp.int32, (LANES, LANES), 1)

    def window(ref, group, first, count):
        return ref[group, first : first + count, :]

    def boxes(group):
        width = group_lanes(
            lambda r: width_ref[pl.ds(core * blocks + r, 1), :], group, per_group
        )
        bits = [width & (1 << e) > 0 for e in range(5)]
        top = slab + 15
        here = window(series_ref, group, 0, top)
        pairs[group, :top, :] = here + window(series_ref, group, 1, top)
        ones[group, :top, :] = jnp.where(bits[0], here, 0.0)
        top = slab + 12
        two = window(pairs, group, 0, top)
        fours[group, :top, :] = two + window(pairs, group, 2, top)
        threes[group, :top, :] = jnp.where(
            bits[1], two + window(ones, group, 2, top), window(ones, group, 0, top)
        )
        sides = []
        for side in range(0, slab, LANES):
            top = LANES + 8
            four = window(fours, group, side, top)
            eight = four + window(fours, group, side + 4, top)
            seven = jnp.where(
                bits[2],
                four + window(threes, group, side + 4, top),
                window(threes, group, side, top),
            )
            some = jnp.where(bits[3], eight[:LANES] + seven[8:], seven[:LANES])
            sides.append(jnp.where(bits[4], eight[:LANES] + eight[8:], some))
        return sides

    for turn in range(groups // cycle):
        moved = [boxes(turn * cycle + q) for q in range(cycle)]
        for j, (start, split) in enumerate(zip(starts, splits)):
            early, late = (
                jnp.where(lane < split, moved[start][side], moved[start + 1][side])
                for side in range(2)
            )
            keep_ref[turn * period + j] = jnp.where(core == 0, early, late)
            send_ref[turn * period + j] = jnp.where(core == 0, late, early)


def box_stage(series, widths, per_group):
    blocks = widths.shape[0] // 2
    return pl.pallas_call(
        functools.partial(box_kernel, per_group),
        out_shape=[jax.ShapeDtypeStruct((blocks, LANES, LANES), jnp.float32)] * 2,
        scratch_shapes=[pltpu.VMEM(series.shape, jnp.float32)] * 4,
        compiler_params=pltpu.CompilerParams(vmem_limit_bytes=12 << 20),
        cost_estimate=COST,
        name="box",
    )(series, widths)


def pair_kernel(own_ref, other_ref, out_ref):
    half = own_ref.shape[0] // 2
    own, other = own_ref[...], other_ref[...]
    first = lax.axis_index("core") == 0
    low = jnp.where(first, own, other)
    high = jnp.where(first, other, own)
    both = jnp.concatenate([low[:half], high[:half], low[half:], high[half:]], 0)
    out_ref[...] = jnp.broadcast_to(both[None], out_ref.shape)


def pair_stage(own, other, peers):
    return pl.pallas_call(
        pair_kernel,
        out_shape=jax.ShapeDtypeStruct((peers, 2 * own.shape[0], LANES), jnp.float32),
        compiler_params=pltpu.CompilerParams(vmem_limit_bytes=8 << 20),
        name="pair",
    )(own, other)


def snr_kernel(samples, period, keep_ref, came_ref, stat_ref, width_ref, out_hbm, done, levels, sems):
    sources, stat_rows, _ = stat_ref.shape
    blocks = stat_rows // 2
    half = blocks // 2
    turns = half // period
    own = samples // sources
    totals = stat_ref[:, :blocks, :]
    average = jnp.sum(totals, 0) * (1.0 / samples)
    apart = totals * (1.0 / own) - average[None]
    squares = jnp.sum(stat_ref[:, blocks:, :], 0) + own * jnp.sum(apart * apart, 0)
    variance = squares * (1.0 / samples)
    width = jnp.concatenate(
        [width_ref[pl.ds(c * half + j, turns, period), :] for c in range(2) for j in range(period)], 0
    )
    width = width.astype(jnp.float32)
    levels[0] = width * average
    levels[1] = lax.rsqrt(width * (variance + 1e-05))
    core = lax.axis_index("core")
    copies = []
    for order, (box_ref, place) in enumerate(((keep_ref, core), (came_ref, 1 - core))):
        for block in range(half):
            row = place * half + block % period * turns + block // period
            at = order * half + block
            level = levels[0, pl.ds(row, 1), :]
            scale = levels[1, pl.ds(row, 1), :]
            done[at * LANES : (at + 1) * LANES, :] = ((box_ref[block] - level) * scale).T
            if (block + 1) % OUT_BLOCKS == 0:
                size = OUT_BLOCKS * LANES
                target = pl.multiple_of((place * half + block + 1 - OUT_BLOCKS) * LANES, LANES)
                copy = pltpu.make_async_copy(
                    done.at[(at + 1) * LANES - size : (at + 1) * LANES, :],
                    out_hbm.at[pl.ds(target, size), :],
                    sems.at[at // OUT_BLOCKS],
                )
                copy.start()
                copies.append(copy)
    for copy in copies:
        copy.wait()


def snr_stage(keep, came, stats, widths, samples, period):
    blocks = widths.shape[0]
    return pl.pallas_call(
        functools.partial(snr_kernel, samples, period),
        out_shape=jax.ShapeDtypeStruct((blocks * LANES, LANES), jnp.float32),
        out_specs=pl.BlockSpec(memory_space=pltpu.HBM),
        scratch_shapes=[
            pltpu.VMEM((blocks * LANES, LANES), jnp.float32),
            pltpu.VMEM((2, blocks, LANES), jnp.float32),
            pltpu.SemaphoreType.DMA((blocks // OUT_BLOCKS,)),
        ],
        compiler_params=pltpu.CompilerParams(vmem_limit_bytes=8 << 20),
        name="snr",
    )(keep, came, stats, widths)


def per_device(filterbank, chan_delay, sub_delay, widths):
    samples = filterbank.shape[1]
    groups = chan_delay.shape[0]
    per_group = sub_delay.shape[0] // groups
    chips, cores = lax.axis_size("chip"), lax.axis_size("core")
    widths = widths.reshape(-1, LANES)
    sent = band_stage(filterbank, chan_delay, chips * cores)
    held = lax.all_to_all(sent, ("chip", "core"), split_axis=0, concat_axis=0, tiled=True)
    series, stats = series_stage(held, sub_delay.T, groups)
    swap = [(0, 1), (1, 0)]
    other = lax.ppermute(stats, "core", swap)
    keep, send = box_stage(series, widths, per_group)
    other, send = lax.optimization_barrier((other, send))
    came = lax.ppermute(send, "core", swap)
    stats = pair_stage(stats, other, chips)
    stats = lax.all_to_all(stats, "chip", split_axis=0, concat_axis=0, tiled=True)
    return snr_stage(keep, came, stats, widths, samples, pieces_of(per_group)[0])


def solution(mesh):
    beams, devices = mesh.devices.shape
    split = jax.sharding.Mesh(
        mesh.devices.reshape(beams, devices // 2, 2), ("beam", "chip", "core")
    )
    lines = ("chip", "core")
    in_specs = (P(("beam", *lines), None), P(None, lines), P(), P())
    out_specs = P("beam", lines)
    return jax.shard_map(
        per_device, mesh=split, in_specs=in_specs, out_specs=out_specs, check_vma=False
    )
```

```python
import functools
import math

import jax
import jax.numpy as jnp
from jax import lax
from jax.experimental import pallas as pl
from jax.experimental.pallas import tpu as pltpu
from jax.sharding import PartitionSpec as P

SUBCH = 32
DELAY_ONE = 8
DELAY_TWO = 16
WMAX = 16
LANES = 128
HALO = 32
NEAR = 2
FAR = DELAY_TWO // 2
FETCHES = 1
OUT_BLOCKS = 2
PACE = 4
COST = pl.CostEstimate(flops=1 << 28, bytes_accessed=1 << 20, transcendentals=0)


def ring_place(chip, chips):
    lines = max(n for n in range(1, math.isqrt(chips) + 1) if chips % n == 0)
    length = chips // lines
    along, line = chip // lines, chip % lines
    return line * length + along + line % 2 * (length - 1 - 2 * along)


def ring_of(chips, cores):
    order = sorted(range(chips), key=lambda chip: ring_place(chip, chips))
    return [chip * cores + core for chip in order for core in range(cores)]


def band_kernel(sub_count, groups, run, fb_hbm, delay_hbm, out_ref, held, delays_ref, carry, tile, sems):
    slabs = out_ref.shape[0]
    channels, samples = fb_hbm.shape
    rows = sub_count * groups
    fetch_delays = pltpu.make_async_copy(delay_hbm, delays_ref, sems.at[0])
    piece = samples // FETCHES
    fetches = [
        pltpu.make_async_copy(
            fb_hbm.at[:, p * piece : (p + 1) * piece],
            held.at[:, p * piece : (p + 1) * piece],
            sems.at[p + 1],
        )
        for p in range(FETCHES)
    ]
    fetch_delays.start()
    for fetch in reversed(fetches):
        fetch.start()
    held[:, samples:] = jnp.zeros((channels, LANES), held.dtype)
    carry[...] = jnp.zeros(carry.shape, carry.dtype)
    part = rows // 2
    for core in range(2):
        last = 2 * ring_place(slabs // 2 - 1, slabs // 2)
        out_ref[last + core, rows:, :] = jnp.zeros((rows // 8, LANES), out_ref.dtype)
    fetch_delays.wait()
    delays = delays_ref[...]
    band_of = lax.broadcasted_iota(jnp.int32, delays.shape, 1) // SUBCH
    hot = []
    for far in range(0, DELAY_ONE, NEAR):
        for core in range(2):
            wanted = delays[core * groups // 2 : (core + 1) * groups // 2]
            for band in range(sub_count):
                mine = band_of[: groups // 2] == band
                hot.append(
                    jnp.concatenate(
                        [
                            jnp.where((wanted == far + near) & mine, 1.0, 0.0)
                            for near in range(NEAR)
                        ],
                        1,
                    )
                )
    hot = jnp.concatenate(hot, 0).astype(jnp.bfloat16)
    lane = lax.broadcasted_iota(jnp.int32, (channels, LANES), 1)
    out_lane = lax.broadcasted_iota(jnp.int32, (rows, LANES), 1)
    place = lax.broadcasted_iota(jnp.int32, (4 * LANES, LANES), 0)
    place_out = lax.broadcasted_iota(jnp.int32, (4 * LANES, LANES), 1)
    fold = (place % LANES < HALO) & (place // LANES * HALO + place % LANES == place_out)
    fold = jnp.where(fold, 1.0, 0.0)
    for fetch in fetches:
        fetch.wait()

    pace = math.gcd(run, PACE)

    def turn(i, _):
        first = (slabs // run - 1 - i) * run

        def tile_at(j):
            return held[:, pl.ds(pl.multiple_of((first + j) * LANES, LANES), LANES)]

        def turned_all(j):
            block = tile_at(j)
            return [block] + [pltpu.roll(block, LANES - near, 1) for near in range(1, NEAR)]

        following = [jnp.zeros((channels, LANES), held.dtype)] * NEAR if run == slabs else turned_all(run)
        late = [carry[far] for far in range(DELAY_ONE // NEAR - 1)]
        for pack in range(run // pace - 1, -1, -1):
            sides = [None] * pace
            for side in range(pace - 1, -1, -1):
                here = turned_all(pace * pack + side)
                sides[side] = jnp.concatenate(
                    [here[0]]
                    + [
                        jnp.where(lane < LANES - near, here[near], following[near])
                        for near in range(1, NEAR)
                    ],
                    0,
                )
                following = here
            parts = jnp.dot(hot, jnp.concatenate(sides, 1), preferred_element_type=jnp.float32)
            for side in range(pace - 1, -1, -1):
                here = parts[:, side * LANES : (side + 1) * LANES]
                total = here[:rows]
                for far in range(1, DELAY_ONE // NEAR):
                    keep = LANES - far * NEAR
                    fresh = pltpu.roll(here[far * rows : (far + 1) * rows], keep, 1)
                    total = total + jnp.where(out_lane < keep, fresh, late[far - 1])
                    late[far - 1] = fresh
                total = total.astype(jnp.bfloat16)
                slot = pace * pack + side
                lead = 2 * ring_place(first // 2 + slot // 2, slabs // 2)
                low = slot % 2 * part
                for core in range(2):
                    out_ref[lead + core, low : low + part, :] = total[core * part : (core + 1) * part]
                if slot % 2 == 0:
                    at = slot // 2 * rows
                    tile[at : at + rows, :] = total.astype(jnp.float32)
        ends = jnp.concatenate(
            [tile[pl.ds(q, run * rows // 8, 4), :] for q in range(4)], 1
        )
        ends = jnp.dot(ends, fold, preferred_element_type=jnp.float32)
        for pair in range(run // 2):
            for core in range(2):
                at = (2 * pair + core) * rows // 8
                end = ends[at : at + rows // 8].astype(out_ref.dtype)
                if pair:
                    lead = 2 * ring_place(first // 2 + pair - 1, slabs // 2)
                    out_ref[lead + core, rows:, :] = end
                else:
                    @pl.when(first > 0)
                    def _():
                        lead = 2 * ring_place(jnp.maximum(first // 2 - 1, 0), slabs // 2)
                        out_ref[lead + core, rows:, :] = end
        for far, block in enumerate(late):
            carry[far] = block
        return 0

    if run == slabs:
        turn(0, 0)
    else:
        lax.fori_loop(0, slabs // run, turn, 0)


def band_stage(filterbank, chan_delay, slabs):
    groups = chan_delay.shape[0]
    channels, samples = filterbank.shape
    rows = channels // SUBCH * groups
    run = math.gcd(slabs, 16)
    return pl.pallas_call(
        functools.partial(band_kernel, channels // SUBCH, groups, run),
        out_shape=jax.ShapeDtypeStruct((slabs, rows + rows // 8, LANES), jnp.bfloat16),
        in_specs=[pl.BlockSpec(memory_space=pltpu.HBM)] * 2,
        scratch_shapes=[
            pltpu.VMEM((channels, samples + LANES), jnp.bfloat16),
            pltpu.VMEM(chan_delay.shape, jnp.int32),
            pltpu.VMEM((DELAY_ONE // NEAR - 1, rows, LANES), jnp.float32),
            pltpu.VMEM((run * rows // 2, LANES), jnp.float32),
            pltpu.SemaphoreType.DMA((FETCHES + 1,)),
        ],
        compiler_params=pltpu.CompilerParams(vmem_limit_bytes=(8 << 20) + 2 * filterbank.size),
        name="bands",
    )(*(pltpu.with_memory_space_constraint(x, pltpu.HBM) for x in (filterbank, chan_delay)))


def group_lanes(block_rows, group, per_group):
    start = group * per_group
    first, shift = start // LANES, start % LANES
    front = block_rows(first)
    if shift + per_group <= LANES:
        return front
    lane = lax.broadcasted_iota(jnp.int32, front.shape, 1)
    return jnp.where(lane < shift, block_rows(first + 1), front)


def one_hot(delays, first, count):
    return jnp.concatenate([jnp.where(delays == first + e, 1.0, 0.0) for e in range(count)], 0)


def pieces_of(per_group):
    period = per_group // HALO
    starts = [LANES * m // per_group for m in range(period)]
    splits = [per_group * (g + 1) - LANES * m for m, g in enumerate(starts)]
    return period, starts, splits


def series_kernel(whole, per_group, held_ref, delay_ref, series_ref, stat_ref, wide, slid, dense, near, rows_at):
    sources, row_count, _ = held_ref.shape
    groups = series_ref.shape[0]
    bands, trials = delay_ref.shape
    per_source = bands // sources
    part = per_source * groups
    blocks = trials // 2 // LANES
    pitch = row_count + 1
    copies = max(1, LANES // bands)
    slab = 2 * LANES
    span = slab + WMAX
    base = 8
    lead = lax.axis_index("core") * blocks
    for block in range(blocks):
        at = pl.multiple_of((lead + block) * LANES, LANES)
        dense[block] = delay_ref[:, pl.ds(at, LANES)]

    def ordered(block):
        return jnp.concatenate(
            [dense[block, pl.ds(b, sources, per_source), :] for b in range(per_source)], 0
        )

    for group in range(groups):
        near[group] = group_lanes(ordered, group, per_group)
    for source in range(sources):
        came = 2 * ring_place(source // 2, sources // 2) + source % 2
        wide[source * pitch : source * pitch + row_count, :] = held_ref[came].astype(jnp.float32)

    def turned(first_row, stride):
        picked = [
            wide[pl.ds(first_row + b * stride, sources, pitch), :] for b in range(per_source)
        ]
        return jnp.concatenate(picked * copies, 0).T

    def store(q, first, block):
        slid[q, base + first : base + first + block.shape[0], :] = block

    def store_slid(q, first, block):
        for copy in range(1, copies):
            low = copy * bands
            top = low + bands
            begin = base + first - copy
            slid[q, begin : begin + block.shape[0], low:top] = block[:, low:top]

    def quad_of(quad, at):
        tails = turned(2 * part + quad, groups // 4)
        for q in range(4):
            group = quad * 4 + q
            place = at + q
            pieces = [turned(side * part + group, groups) for side in range(2)]
            pieces.append(tails[q * HALO : (q + 1) * HALO])
            for side, piece in enumerate(pieces):
                store(place, side * LANES, piece)
            for side, piece in enumerate(pieces):
                store_slid(place, side * LANES, piece)
            both = jnp.zeros((span + FAR, 2 * LANES), jnp.float32)
            step = 2 * copies
            for offset in range(0, FAR, step):
                hot = jnp.concatenate(
                    [one_hot(near[group], far + offset, step) for far in (0, FAR)], 1
                )
                left = jnp.concatenate(
                    [
                        slid[place, base + o : base + o + span + FAR, :]
                        for o in range(offset, offset + step, copies)
                    ],
                    1,
                )
                both = both + jnp.dot(left, hot, preferred_element_type=jnp.float32)
            out = both[:span, :LANES] + both[FAR:, LANES:]
            series_ref[group] = out
            own = out[:slab]
            total = jnp.sum(own, 0, keepdims=True)
            centred = own - total * (1.0 / slab)
            rows_at[0, pl.ds(group, 1), :] = total
            rows_at[1, pl.ds(group, 1), :] = jnp.sum(centred * centred, 0, keepdims=True)

    if whole:
        for quad in range(groups // 4):
            quad_of(quad, quad * 4)
    else:

        def turn(quad, _):
            quad_of(quad, 0)
            return 0

        lax.fori_loop(0, groups // 4, turn, 0)

    period, starts, splits = pieces_of(per_group)
    cycle = period + 1
    lane = lax.broadcasted_iota(jnp.int32, (groups // cycle, LANES), 1)
    packed = []
    for stat in range(2):
        moved = [rows_at[stat, pl.ds(q, groups // cycle, cycle), :] for q in range(cycle)]
        for start, split in zip(starts, splits):
            packed.append(jnp.where(lane < split, moved[start], moved[start + 1]))
    stat_ref[...] = jnp.concatenate(packed, 0)


def series_stage(held, delays, groups):
    sources, row_count, _ = held.shape
    bands, trials = delays.shape
    across = max(LANES, bands)
    whole = bands <= LANES
    half = groups // 2
    return pl.pallas_call(
        functools.partial(series_kernel, whole, trials // groups),
        out_shape=(
            jax.ShapeDtypeStruct((half, 2 * LANES + WMAX, LANES), jnp.float32),
            jax.ShapeDtypeStruct((trials // LANES, LANES), jnp.float32),
        ),
        scratch_shapes=[
            pltpu.VMEM((sources * (row_count + 1) + 7, LANES), jnp.float32),
            pltpu.VMEM((half if whole else 4, 2 * LANES + HALO + 8, across), jnp.float32),
            pltpu.VMEM((trials // 2 // LANES, bands, LANES), jnp.int32),
            pltpu.VMEM((half, bands, LANES), jnp.int32),
            pltpu.VMEM((2, half, LANES), jnp.float32),
        ],
        compiler_params=pltpu.CompilerParams(
            vmem_limit_bytes=(8 << 20) + (0 if whole else 32 << 20),
        ),
        name="series",
    )(held, delays)


def box_kernel(per_group, series_ref, width_ref, keep_ref, send_ref, pairs, ones, fours, threes):
    groups = series_ref.shape[0]
    slab = 2 * LANES
    period, starts, splits = pieces_of(per_group)
    cycle = period + 1
    blocks = keep_ref.shape[0]
    core = lax.axis_index("core")
    lane = lax.broadcasted_iota(jnp.int32, (LANES, LANES), 1)

    def window(ref, group, first, count):
        return ref[group, first : first + count, :]

    def boxes(group):
        width = group_lanes(
            lambda r: width_ref[pl.ds(core * blocks + r, 1), :], group, per_group
        )
        bits = [width & (1 << e) > 0 for e in range(5)]
        top = slab + 15
        here = window(series_ref, group, 0, top)
        pairs[group, :top, :] = here + window(series_ref, group, 1, top)
        ones[group, :top, :] = jnp.where(bits[0], here, 0.0)
        top = slab + 12
        two = window(pairs, group, 0, top)
        fours[group, :top, :] = two + window(pairs, group, 2, top)
        threes[group, :top, :] = jnp.where(
            bits[1], two + window(ones, group, 2, top), window(ones, group, 0, top)
        )
        sides = []
        for side in range(0, slab, LANES):
            top = LANES + 8
            four = window(fours, group, side, top)
            eight = four + window(fours, group, side + 4, top)
            seven = jnp.where(
                bits[2],
                four + window(threes, group, side + 4, top),
                window(threes, group, side, top),
            )
            some = jnp.where(bits[3], eight[:LANES] + seven[8:], seven[:LANES])
            sides.append(jnp.where(bits[4], eight[:LANES] + eight[8:], some))
        return sides

    for turn in range(groups // cycle):
        moved = [boxes(turn * cycle + q) for q in range(cycle)]
        for j, (start, split) in enumerate(zip(starts, splits)):
            early, late = (
                jnp.where(lane < split, moved[start][side], moved[start + 1][side])
                for side in range(2)
            )
            keep_ref[turn * period + j] = jnp.where(core == 0, early, late)
            send_ref[turn * period + j] = jnp.where(core == 0, late, early)


def box_stage(series, widths, per_group):
    blocks = widths.shape[0] // 2
    return pl.pallas_call(
        functools.partial(box_kernel, per_group),
        out_shape=[jax.ShapeDtypeStruct((blocks, LANES, LANES), jnp.float32)] * 2,
        scratch_shapes=[pltpu.VMEM(series.shape, jnp.float32)] * 4,
        compiler_params=pltpu.CompilerParams(vmem_limit_bytes=12 << 20),
        cost_estimate=COST,
        name="box",
    )(series, widths)


def pair_kernel(own_ref, other_ref, out_ref):
    half = own_ref.shape[0] // 2
    own, other = own_ref[...], other_ref[...]
    first = lax.axis_index("core") == 0
    low = jnp.where(first, own, other)
    high = jnp.where(first, other, own)
    both = jnp.concatenate([low[:half], high[:half], low[half:], high[half:]], 0)
    out_ref[...] = jnp.broadcast_to(both[None], out_ref.shape)


def pair_stage(own, other, peers):
    return pl.pallas_call(
        pair_kernel,
        out_shape=jax.ShapeDtypeStruct((peers, 2 * own.shape[0], LANES), jnp.float32),
        compiler_params=pltpu.CompilerParams(vmem_limit_bytes=8 << 20),
        name="pair",
    )(own, other)


def snr_kernel(samples, period, keep_ref, came_ref, stat_ref, width_ref, out_hbm, done, levels, sems):
    sources, stat_rows, _ = stat_ref.shape
    blocks = stat_rows // 2
    half = blocks // 2
    turns = half // period
    own = samples // sources
    totals = stat_ref[:, :blocks, :]
    average = jnp.sum(totals, 0) * (1.0 / samples)
    apart = totals * (1.0 / own) - average[None]
    squares = jnp.sum(stat_ref[:, blocks:, :], 0) + own * jnp.sum(apart * apart, 0)
    variance = squares * (1.0 / samples)
    width = jnp.concatenate(
        [width_ref[pl.ds(c * half + j, turns, period), :] for c in range(2) for j in range(period)], 0
    )
    width = width.astype(jnp.float32)
    levels[0] = width * average
    levels[1] = lax.rsqrt(width * (variance + 1e-05))
    core = lax.axis_index("core")
    copies = []
    for order, (box_ref, place) in enumerate(((keep_ref, core), (came_ref, 1 - core))):
        for block in range(half):
            row = place * half + block % period * turns + block // period
            at = order * half + block
            level = levels[0, pl.ds(row, 1), :]
            scale = levels[1, pl.ds(row, 1), :]
            done[at * LANES : (at + 1) * LANES, :] = ((box_ref[block] - level) * scale).T
            if (block + 1) % OUT_BLOCKS == 0:
                size = OUT_BLOCKS * LANES
                target = pl.multiple_of((place * half + block + 1 - OUT_BLOCKS) * LANES, LANES)
                copy = pltpu.make_async_copy(
                    done.at[(at + 1) * LANES - size : (at + 1) * LANES, :],
                    out_hbm.at[pl.ds(target, size), :],
                    sems.at[at // OUT_BLOCKS],
                )
                copy.start()
                copies.append(copy)
    for copy in copies:
        copy.wait()


def snr_stage(keep, came, stats, widths, samples, period):
    blocks = widths.shape[0]
    return pl.pallas_call(
        functools.partial(snr_kernel, samples, period),
        out_shape=jax.ShapeDtypeStruct((blocks * LANES, LANES), jnp.float32),
        out_specs=pl.BlockSpec(memory_space=pltpu.HBM),
        scratch_shapes=[
            pltpu.VMEM((blocks * LANES, LANES), jnp.float32),
            pltpu.VMEM((2, blocks, LANES), jnp.float32),
            pltpu.SemaphoreType.DMA((blocks // OUT_BLOCKS,)),
        ],
        compiler_params=pltpu.CompilerParams(vmem_limit_bytes=8 << 20),
        name="snr",
    )(keep, came, stats, widths)


def per_device(filterbank, chan_delay, sub_delay, widths):
    samples = filterbank.shape[1]
    groups = chan_delay.shape[0]
    per_group = sub_delay.shape[0] // groups
    chips, cores = lax.axis_size("chip"), lax.axis_size("core")
    widths = widths.reshape(-1, LANES)
    sent = band_stage(filterbank, chan_delay, chips * cores)
    held = lax.all_to_all(
        sent,
        ("chip", "core"),
        split_axis=0,
        concat_axis=0,
        tiled=True,
        axis_index_groups=[ring_of(chips, cores)],
    )
    series, stats = series_stage(held, sub_delay.T, groups)
    swap = [(0, 1), (1, 0)]
    other = lax.ppermute(stats, "core", swap)
    keep, send = box_stage(series, widths, per_group)
    other, send = lax.optimization_barrier((other, send))
    came = lax.ppermute(send, "core", swap)
    stats = pair_stage(stats, other, chips)
    stats = lax.all_to_all(
        stats,
        "chip",
        split_axis=0,
        concat_axis=0,
        tiled=True,
        axis_index_groups=[ring_of(chips, 1)],
    )
    return snr_stage(keep, came, stats, widths, samples, pieces_of(per_group)[0])


def solution(mesh):
    beams, devices = mesh.devices.shape
    split = jax.sharding.Mesh(
        mesh.devices.reshape(beams, devices // 2, 2), ("beam", "chip", "core")
    )
    lines = ("chip", "core")
    in_specs = (P(("beam", *lines), None), P(None, lines), P(), P())
    out_specs = P("beam", lines)
    return jax.shard_map(
        per_device, mesh=split, in_specs=in_specs, out_specs=out_specs, check_vma=False
    )
```

```python
import functools
import math

import jax
import jax.numpy as jnp
from jax import lax
from jax.experimental import pallas as pl
from jax.experimental.pallas import tpu as pltpu
from jax.sharding import PartitionSpec as P

SUBCH = 32
DELAY_ONE = 8
DELAY_TWO = 16
WMAX = 16
LANES = 128
HALO = 32
NEAR = 2
FAR = DELAY_TWO // 2
FETCHES = 1
OUT_BLOCKS = 2
PACE = 4
COST = pl.CostEstimate(flops=1 << 28, bytes_accessed=1 << 20, transcendentals=0)


def ring_place(chip, chips):
    lines = max(n for n in range(1, math.isqrt(chips) + 1) if chips % n == 0)
    length = chips // lines
    along, line = chip // lines, chip % lines
    return line * length + along + line % 2 * (length - 1 - 2 * along)


def ring_of(chips, cores):
    order = sorted(range(chips), key=lambda chip: ring_place(chip, chips))
    return [chip * cores + core for chip in order for core in range(cores)]


def band_kernel(sub_count, groups, run, fb_hbm, delay_hbm, out_ref, held, delays_ref, carry, tile, sems):
    slabs = out_ref.shape[0]
    channels, samples = fb_hbm.shape
    rows = sub_count * groups
    fetch_delays = pltpu.make_async_copy(delay_hbm, delays_ref, sems.at[0])
    piece = samples // FETCHES
    fetches = [
        pltpu.make_async_copy(
            fb_hbm.at[:, p * piece : (p + 1) * piece],
            held.at[:, p * piece : (p + 1) * piece],
            sems.at[p + 1],
        )
        for p in range(FETCHES)
    ]
    fetch_delays.start()
    for fetch in reversed(fetches):
        fetch.start()
    held[:, samples:] = jnp.zeros((channels, LANES), held.dtype)
    carry[...] = jnp.zeros(carry.shape, carry.dtype)
    part = rows // 2
    for core in range(2):
        last = 2 * ring_place(slabs // 2 - 1, slabs // 2)
        out_ref[last + core, rows:, :] = jnp.zeros((rows // 8, LANES), out_ref.dtype)
    fetch_delays.wait()
    delays = delays_ref[...]
    band_of = lax.broadcasted_iota(jnp.int32, delays.shape, 1) // SUBCH
    hot = []
    for far in range(0, DELAY_ONE, NEAR):
        for core in range(2):
            wanted = delays[core * groups // 2 : (core + 1) * groups // 2]
            for band in range(sub_count):
                mine = band_of[: groups // 2] == band
                hot.append(
                    jnp.concatenate(
                        [
                            jnp.where((wanted == far + near) & mine, 1.0, 0.0)
                            for near in range(NEAR)
                        ],
                        1,
                    )
                )
    hot = jnp.concatenate(hot, 0).astype(jnp.bfloat16)
    lane = lax.broadcasted_iota(jnp.int32, (channels, LANES), 1)
    out_lane = lax.broadcasted_iota(jnp.int32, (rows, LANES), 1)
    place = lax.broadcasted_iota(jnp.int32, (4 * LANES, LANES), 0)
    place_out = lax.broadcasted_iota(jnp.int32, (4 * LANES, LANES), 1)
    fold = (place % LANES < HALO) & (place // LANES * HALO + place % LANES == place_out)
    fold = jnp.where(fold, 1.0, 0.0)
    for fetch in fetches:
        fetch.wait()

    pace = math.gcd(run, PACE)

    def turn(i, _):
        first = (slabs // run - 1 - i) * run

        def tile_at(j):
            return held[:, pl.ds(pl.multiple_of((first + j) * LANES, LANES), LANES)]

        def turned_all(j):
            block = tile_at(j)
            return [block] + [pltpu.roll(block, LANES - near, 1) for near in range(1, NEAR)]

        following = [jnp.zeros((channels, LANES), held.dtype)] * NEAR if run == slabs else turned_all(run)
        late = [carry[far] for far in range(DELAY_ONE // NEAR - 1)]
        for pack in range(run // pace - 1, -1, -1):
            sides = [None] * pace
            for side in range(pace - 1, -1, -1):
                here = turned_all(pace * pack + side)
                sides[side] = jnp.concatenate(
                    [here[0]]
                    + [
                        jnp.where(lane < LANES - near, here[near], following[near])
                        for near in range(1, NEAR)
                    ],
                    0,
                )
                following = here
            parts = jnp.dot(hot, jnp.concatenate(sides, 1), preferred_element_type=jnp.float32)
            for side in range(pace - 1, -1, -1):
                here = parts[:, side * LANES : (side + 1) * LANES]
                total = here[:rows]
                for far in range(1, DELAY_ONE // NEAR):
                    keep = LANES - far * NEAR
                    fresh = pltpu.roll(here[far * rows : (far + 1) * rows], keep, 1)
                    total = total + jnp.where(out_lane < keep, fresh, late[far - 1])
                    late[far - 1] = fresh
                total = total.astype(jnp.bfloat16)
                slot = pace * pack + side
                lead = 2 * ring_place(first // 2 + slot // 2, slabs // 2)
                low = slot % 2 * part
                for core in range(2):
                    out_ref[lead + core, low : low + part, :] = total[core * part : (core + 1) * part]
                if slot % 2 == 0:
                    at = slot // 2 * rows
                    tile[at : at + rows, :] = total.astype(jnp.float32)
        ends = jnp.concatenate(
            [tile[pl.ds(q, run * rows // 8, 4), :] for q in range(4)], 1
        )
        ends = jnp.dot(ends, fold, preferred_element_type=jnp.float32)
        for pair in range(run // 2):
            for core in range(2):
                at = (2 * pair + core) * rows // 8
                end = ends[at : at + rows // 8].astype(out_ref.dtype)
                if pair:
                    lead = 2 * ring_place(first // 2 + pair - 1, slabs // 2)
                    out_ref[lead + core, rows:, :] = end
                else:
                    @pl.when(first > 0)
                    def _():
                        lead = 2 * ring_place(jnp.maximum(first // 2 - 1, 0), slabs // 2)
                        out_ref[lead + core, rows:, :] = end
        for far, block in enumerate(late):
            carry[far] = block
        return 0

    if run == slabs:
        turn(0, 0)
    else:
        lax.fori_loop(0, slabs // run, turn, 0)


def band_stage(filterbank, chan_delay, slabs):
    groups = chan_delay.shape[0]
    channels, samples = filterbank.shape
    rows = channels // SUBCH * groups
    run = math.gcd(slabs, 16)
    return pl.pallas_call(
        functools.partial(band_kernel, channels // SUBCH, groups, run),
        out_shape=jax.ShapeDtypeStruct((slabs, rows + rows // 8, LANES), jnp.bfloat16),
        in_specs=[pl.BlockSpec(memory_space=pltpu.HBM)] * 2,
        scratch_shapes=[
            pltpu.VMEM((channels, samples + LANES), jnp.bfloat16),
            pltpu.VMEM(chan_delay.shape, jnp.int32),
            pltpu.VMEM((DELAY_ONE // NEAR - 1, rows, LANES), jnp.float32),
            pltpu.VMEM((run * rows // 2, LANES), jnp.float32),
            pltpu.SemaphoreType.DMA((FETCHES + 1,)),
        ],
        compiler_params=pltpu.CompilerParams(vmem_limit_bytes=(8 << 20) + 2 * filterbank.size),
        name="bands",
    )(*(pltpu.with_memory_space_constraint(x, pltpu.HBM) for x in (filterbank, chan_delay)))


def group_lanes(block_rows, group, per_group):
    start = group * per_group
    first, shift = start // LANES, start % LANES
    front = block_rows(first)
    if shift + per_group <= LANES:
        return front
    lane = lax.broadcasted_iota(jnp.int32, front.shape, 1)
    return jnp.where(lane < shift, block_rows(first + 1), front)


def one_hot(delays, first, count):
    return jnp.concatenate([jnp.where(delays == first + e, 1.0, 0.0) for e in range(count)], 0)


def pieces_of(per_group):
    period = per_group // HALO
    starts = [LANES * m // per_group for m in range(period)]
    splits = [per_group * (g + 1) - LANES * m for m, g in enumerate(starts)]
    return period, starts, splits


def series_kernel(whole, per_group, held_ref, delay_ref, series_ref, stat_ref, wide, slid, dense, near, rows_at):
    sources, row_count, _ = held_ref.shape
    groups = series_ref.shape[0]
    bands, trials = delay_ref.shape
    per_source = bands // sources
    part = per_source * groups
    blocks = trials // 2 // LANES
    pitch = row_count + 1
    copies = max(1, LANES // bands)
    slab = 2 * LANES
    span = slab + WMAX
    base = 8
    lead = lax.axis_index("core") * blocks
    for block in range(blocks):
        at = pl.multiple_of((lead + block) * LANES, LANES)
        dense[block] = delay_ref[:, pl.ds(at, LANES)]

    def ordered(block):
        return jnp.concatenate(
            [dense[block, pl.ds(b, sources, per_source), :] for b in range(per_source)], 0
        )

    for group in range(groups):
        near[group] = group_lanes(ordered, group, per_group)
    for source in range(sources):
        came = 2 * ring_place(source // 2, sources // 2) + source % 2
        wide[source * pitch : source * pitch + row_count, :] = held_ref[came].astype(jnp.float32)

    def turned(first_row, stride):
        picked = [
            wide[pl.ds(first_row + b * stride, sources, pitch), :] for b in range(per_source)
        ]
        return jnp.concatenate(picked * copies, 0).T

    def store(q, first, block):
        slid[q, base + first : base + first + block.shape[0], :] = block

    def store_slid(q, first, block):
        for copy in range(1, copies):
            low = copy * bands
            top = low + bands
            begin = base + first - copy
            slid[q, begin : begin + block.shape[0], low:top] = block[:, low:top]

    def quad_of(quad, at):
        tails = turned(2 * part + quad, groups // 4)
        for q in range(4):
            group = quad * 4 + q
            place = at + q
            pieces = [turned(side * part + group, groups) for side in range(2)]
            pieces.append(tails[q * HALO : (q + 1) * HALO])
            for side, piece in enumerate(pieces):
                store(place, side * LANES, piece)
            for side, piece in enumerate(pieces):
                store_slid(place, side * LANES, piece)
            both = jnp.zeros((span + FAR, 2 * LANES), jnp.float32)
            step = 2 * copies
            for offset in range(0, FAR, step):
                hot = jnp.concatenate(
                    [one_hot(near[group], far + offset, step) for far in (0, FAR)], 1
                )
                left = jnp.concatenate(
                    [
                        slid[place, base + o : base + o + span + FAR, :]
                        for o in range(offset, offset + step, copies)
                    ],
                    1,
                )
                both = both + jnp.dot(left, hot, preferred_element_type=jnp.float32)
            out = both[:span, :LANES] + both[FAR:, LANES:]
            series_ref[group] = out
            own = out[:slab]
            total = jnp.sum(own, 0, keepdims=True)
            centred = own - total * (1.0 / slab)
            rows_at[0, pl.ds(group, 1), :] = total
            rows_at[1, pl.ds(group, 1), :] = jnp.sum(centred * centred, 0, keepdims=True)

    if whole:
        for quad in range(groups // 4):
            quad_of(quad, quad * 4)
    else:

        def turn(quad, _):
            quad_of(quad, 0)
            return 0

        lax.fori_loop(0, groups // 4, turn, 0)

    period, starts, splits = pieces_of(per_group)
    cycle = period + 1
    lane = lax.broadcasted_iota(jnp.int32, (groups // cycle, LANES), 1)
    packed = []
    for stat in range(2):
        moved = [rows_at[stat, pl.ds(q, groups // cycle, cycle), :] for q in range(cycle)]
        for start, split in zip(starts, splits):
            packed.append(jnp.where(lane < split, moved[start], moved[start + 1]))
    stat_ref[...] = jnp.concatenate(packed, 0)


def series_stage(held, delays, groups):
    sources, row_count, _ = held.shape
    bands, trials = delays.shape
    across = max(LANES, bands)
    whole = bands <= LANES
    half = groups // 2
    return pl.pallas_call(
        functools.partial(series_kernel, whole, trials // groups),
        out_shape=(
            jax.ShapeDtypeStruct((half, 2 * LANES + WMAX, LANES), jnp.float32),
            jax.ShapeDtypeStruct((trials // LANES, LANES), jnp.float32),
        ),
        scratch_shapes=[
            pltpu.VMEM((sources * (row_count + 1) + 7, LANES), jnp.float32),
            pltpu.VMEM((half if whole else 4, 2 * LANES + HALO + 8, across), jnp.float32),
            pltpu.VMEM((trials // 2 // LANES, bands, LANES), jnp.int32),
            pltpu.VMEM((half, bands, LANES), jnp.int32),
            pltpu.VMEM((2, half, LANES), jnp.float32),
        ],
        compiler_params=pltpu.CompilerParams(
            vmem_limit_bytes=(8 << 20) + (0 if whole else 32 << 20),
        ),
        name="series",
    )(held, delays)


def box_kernel(per_group, series_ref, width_ref, keep_ref, send_ref, pairs, ones, fours, threes):
    groups = series_ref.shape[0]
    slab = 2 * LANES
    period, starts, splits = pieces_of(per_group)
    cycle = period + 1
    blocks = keep_ref.shape[0]
    core = lax.axis_index("core")
    lane = lax.broadcasted_iota(jnp.int32, (LANES, LANES), 1)

    def window(ref, group, first, count):
        return ref[group, first : first + count, :]

    def boxes(group):
        width = group_lanes(
            lambda r: width_ref[pl.ds(core * blocks + r, 1), :], group, per_group
        )
        bits = [width & (1 << e) > 0 for e in range(5)]
        top = slab + 15
        here = window(series_ref, group, 0, top)
        pairs[group, :top, :] = here + window(series_ref, group, 1, top)
        ones[group, :top, :] = jnp.where(bits[0], here, 0.0)
        top = slab + 12
        two = window(pairs, group, 0, top)
        fours[group, :top, :] = two + window(pairs, group, 2, top)
        threes[group, :top, :] = jnp.where(
            bits[1], two + window(ones, group, 2, top), window(ones, group, 0, top)
        )
        sides = []
        for side in range(0, slab, LANES):
            top = LANES + 8
            four = window(fours, group, side, top)
            eight = four + window(fours, group, side + 4, top)
            seven = jnp.where(
                bits[2],
                four + window(threes, group, side + 4, top),
                window(threes, group, side, top),
            )
            some = jnp.where(bits[3], eight[:LANES] + seven[8:], seven[:LANES])
            sides.append(jnp.where(bits[4], eight[:LANES] + eight[8:], some))
        return sides

    for turn in range(groups // cycle):
        moved = [boxes(turn * cycle + q) for q in range(cycle)]
        for j, (start, split) in enumerate(zip(starts, splits)):
            early, late = (
                jnp.where(lane < split, moved[start][side], moved[start + 1][side])
                for side in range(2)
            )
            keep_ref[turn * period + j] = jnp.where(core == 0, early, late)
            send_ref[turn * period + j] = jnp.where(core == 0, late, early)


def box_stage(series, widths, per_group):
    blocks = widths.shape[0] // 2
    return pl.pallas_call(
        functools.partial(box_kernel, per_group),
        out_shape=[jax.ShapeDtypeStruct((blocks, LANES, LANES), jnp.float32)] * 2,
        scratch_shapes=[pltpu.VMEM(series.shape, jnp.float32)] * 4,
        compiler_params=pltpu.CompilerParams(vmem_limit_bytes=12 << 20),
        cost_estimate=COST,
        name="box",
    )(series, widths)


def pair_kernel(own_ref, other_ref, out_ref):
    half = own_ref.shape[0] // 2
    own, other = own_ref[...], other_ref[...]
    first = lax.axis_index("core") == 0
    low = jnp.where(first, own, other)
    high = jnp.where(first, other, own)
    both = jnp.concatenate([low[:half], high[:half], low[half:], high[half:]], 0)
    out_ref[...] = jnp.broadcast_to(both[None], out_ref.shape)


def pair_stage(own, other, peers):
    return pl.pallas_call(
        pair_kernel,
        out_shape=jax.ShapeDtypeStruct((peers, 2 * own.shape[0], LANES), jnp.float32),
        compiler_params=pltpu.CompilerParams(vmem_limit_bytes=8 << 20),
        name="pair",
    )(own, other)


def snr_kernel(samples, period, keep_ref, came_ref, stat_ref, width_ref, out_hbm, done, levels, sems):
    sources, stat_rows, _ = stat_ref.shape
    blocks = stat_rows // 2
    half = blocks // 2
    turns = half // period
    own = samples // sources
    totals = stat_ref[:, :blocks, :]
    average = jnp.sum(totals, 0) * (1.0 / samples)
    apart = totals * (1.0 / own) - average[None]
    squares = jnp.sum(stat_ref[:, blocks:, :], 0) + own * jnp.sum(apart * apart, 0)
    variance = squares * (1.0 / samples)
    width = jnp.concatenate(
        [width_ref[pl.ds(c * half + j, turns, period), :] for c in range(2) for j in range(period)], 0
    )
    width = width.astype(jnp.float32)
    levels[0] = width * average
    levels[1] = lax.rsqrt(width * (variance + 1e-05))
    core = lax.axis_index("core")
    copies = []
    for order, (box_ref, place) in enumerate(((keep_ref, core), (came_ref, 1 - core))):
        for block in range(half):
            row = place * half + block % period * turns + block // period
            at = order * half + block
            level = levels[0, pl.ds(row, 1), :]
            scale = levels[1, pl.ds(row, 1), :]
            done[at * LANES : (at + 1) * LANES, :] = ((box_ref[block] - level) * scale).T
            if (block + 1) % OUT_BLOCKS == 0:
                size = OUT_BLOCKS * LANES
                target = pl.multiple_of((place * half + block + 1 - OUT_BLOCKS) * LANES, LANES)
                copy = pltpu.make_async_copy(
                    done.at[(at + 1) * LANES - size : (at + 1) * LANES, :],
                    out_hbm.at[pl.ds(target, size), :],
                    sems.at[at // OUT_BLOCKS],
                )
                copy.start()
                copies.append(copy)
    for copy in copies:
        copy.wait()


def snr_stage(keep, came, stats, widths, samples, period):
    blocks = widths.shape[0]
    return pl.pallas_call(
        functools.partial(snr_kernel, samples, period),
        out_shape=jax.ShapeDtypeStruct((blocks * LANES, LANES), jnp.float32),
        out_specs=pl.BlockSpec(memory_space=pltpu.HBM),
        scratch_shapes=[
            pltpu.VMEM((blocks * LANES, LANES), jnp.float32),
            pltpu.VMEM((2, blocks, LANES), jnp.float32),
            pltpu.SemaphoreType.DMA((blocks // OUT_BLOCKS,)),
        ],
        compiler_params=pltpu.CompilerParams(vmem_limit_bytes=8 << 20),
        name="snr",
    )(keep, came, stats, widths)


def per_device(filterbank, chan_delay, sub_delay, widths):
    samples = filterbank.shape[1]
    groups = chan_delay.shape[0]
    per_group = sub_delay.shape[0] // groups
    chips, cores = lax.axis_size("chip"), lax.axis_size("core")
    widths = widths.reshape(-1, LANES)
    sent = band_stage(filterbank, chan_delay, chips * cores)
    held = lax.all_to_all(
        sent,
        ("chip", "core"),
        split_axis=0,
        concat_axis=0,
        tiled=True,
        axis_index_groups=[ring_of(chips, cores)],
    )
    series, stats = series_stage(held, sub_delay.T, groups)
    swap = [(0, 1), (1, 0)]
    other = lax.ppermute(stats, "core", swap)
    keep, send = box_stage(series, widths, per_group)
    other, send = lax.optimization_barrier((other, send))
    came = lax.ppermute(send, "core", swap)
    stats = pair_stage(stats, other, chips)
    stats = lax.all_to_all(
        stats,
        "chip",
        split_axis=0,
        concat_axis=0,
        tiled=True,
    )
    return snr_stage(keep, came, stats, widths, samples, pieces_of(per_group)[0])


def solution(mesh):
    beams, devices = mesh.devices.shape
    split = jax.sharding.Mesh(
        mesh.devices.reshape(beams, devices // 2, 2), ("beam", "chip", "core")
    )
    lines = ("chip", "core")
    in_specs = (P(("beam", *lines), None), P(None, lines), P(), P())
    out_specs = P("beam", lines)
    return jax.shard_map(
        per_device, mesh=split, in_specs=in_specs, out_specs=out_specs, check_vma=False
    )
```

```python
import functools
import math

import jax
import jax.numpy as jnp
from jax import lax
from jax.experimental import pallas as pl
from jax.experimental.pallas import tpu as pltpu
from jax.sharding import PartitionSpec as P

SUBCH = 32
DELAY_ONE = 8
DELAY_TWO = 16
WMAX = 16
LANES = 128
HALO = 32
NEAR = 2
FAR = DELAY_TWO // 2
FETCHES = 1
OUT_BLOCKS = 3
PACE = 4
COST = pl.CostEstimate(flops=1 << 28, bytes_accessed=1 << 20, transcendentals=0)


def ring_place(chip, chips):
    lines = max(n for n in range(1, math.isqrt(chips) + 1) if chips % n == 0)
    length = chips // lines
    along, line = chip // lines, chip % lines
    return line * length + along + line % 2 * (length - 1 - 2 * along)


def ring_of(chips, cores):
    order = sorted(range(chips), key=lambda chip: ring_place(chip, chips))
    return [chip * cores + core for chip in order for core in range(cores)]


def band_kernel(sub_count, groups, run, fb_hbm, delay_hbm, out_ref, held, delays_ref, carry, tile, sems):
    slabs = out_ref.shape[0]
    channels, samples = fb_hbm.shape
    rows = sub_count * groups
    fetch_delays = pltpu.make_async_copy(delay_hbm, delays_ref, sems.at[0])
    piece = samples // FETCHES
    fetches = [
        pltpu.make_async_copy(
            fb_hbm.at[:, p * piece : (p + 1) * piece],
            held.at[:, p * piece : (p + 1) * piece],
            sems.at[p + 1],
        )
        for p in range(FETCHES)
    ]
    fetch_delays.start()
    for fetch in reversed(fetches):
        fetch.start()
    held[:, samples:] = jnp.zeros((channels, LANES), held.dtype)
    carry[...] = jnp.zeros(carry.shape, carry.dtype)
    part = rows // 2
    for core in range(2):
        last = 2 * ring_place(slabs // 2 - 1, slabs // 2)
        out_ref[last + core, rows:, :] = jnp.zeros((rows // 8, LANES), out_ref.dtype)
    fetch_delays.wait()
    delays = delays_ref[...]
    band_of = lax.broadcasted_iota(jnp.int32, delays.shape, 1) // SUBCH
    hot = []
    for far in range(0, DELAY_ONE, NEAR):
        for core in range(2):
            wanted = delays[core * groups // 2 : (core + 1) * groups // 2]
            for band in range(sub_count):
                mine = band_of[: groups // 2] == band
                hot.append(
                    jnp.concatenate(
                        [
                            jnp.where((wanted == far + near) & mine, 1.0, 0.0)
                            for near in range(NEAR)
                        ],
                        1,
                    )
                )
    hot = jnp.concatenate(hot, 0).astype(jnp.bfloat16)
    lane = lax.broadcasted_iota(jnp.int32, (channels, LANES), 1)
    out_lane = lax.broadcasted_iota(jnp.int32, (rows, LANES), 1)
    place = lax.broadcasted_iota(jnp.int32, (4 * LANES, LANES), 0)
    place_out = lax.broadcasted_iota(jnp.int32, (4 * LANES, LANES), 1)
    fold = (place % LANES < HALO) & (place // LANES * HALO + place % LANES == place_out)
    fold = jnp.where(fold, 1.0, 0.0)
    for fetch in fetches:
        fetch.wait()

    pace = math.gcd(run, PACE)

    def turn(i, _):
        first = (slabs // run - 1 - i) * run

        def tile_at(j):
            return held[:, pl.ds(pl.multiple_of((first + j) * LANES, LANES), LANES)]

        def turned_all(j):
            block = tile_at(j)
            return [block] + [pltpu.roll(block, LANES - near, 1) for near in range(1, NEAR)]

        following = [jnp.zeros((channels, LANES), held.dtype)] * NEAR if run == slabs else turned_all(run)
        late = [carry[far] for far in range(DELAY_ONE // NEAR - 1)]
        for pack in range(run // pace - 1, -1, -1):
            sides = [None] * pace
            for side in range(pace - 1, -1, -1):
                here = turned_all(pace * pack + side)
                sides[side] = jnp.concatenate(
                    [here[0]]
                    + [
                        jnp.where(lane < LANES - near, here[near], following[near])
                        for near in range(1, NEAR)
                    ],
                    0,
                )
                following = here
            parts = jnp.dot(hot, jnp.concatenate(sides, 1), preferred_element_type=jnp.float32)
            for side in range(pace - 1, -1, -1):
                here = parts[:, side * LANES : (side + 1) * LANES]
                total = here[:rows]
                for far in range(1, DELAY_ONE // NEAR):
                    keep = LANES - far * NEAR
                    fresh = pltpu.roll(here[far * rows : (far + 1) * rows], keep, 1)
                    total = total + jnp.where(out_lane < keep, fresh, late[far - 1])
                    late[far - 1] = fresh
                total = total.astype(jnp.bfloat16)
                slot = pace * pack + side
                lead = 2 * ring_place(first // 2 + slot // 2, slabs // 2)
                low = slot % 2 * part
                for core in range(2):
                    out_ref[lead + core, low : low + part, :] = total[core * part : (core + 1) * part]
                if slot % 2 == 0:
                    at = slot // 2 * rows
                    tile[at : at + rows, :] = total.astype(jnp.float32)
        ends = jnp.concatenate(
            [tile[pl.ds(q, run * rows // 8, 4), :] for q in range(4)], 1
        )
        ends = jnp.dot(ends, fold, preferred_element_type=jnp.float32)
        for pair in range(run // 2):
            for core in range(2):
                at = (2 * pair + core) * rows // 8
                end = ends[at : at + rows // 8].astype(out_ref.dtype)
                if pair:
                    lead = 2 * ring_place(first // 2 + pair - 1, slabs // 2)
                    out_ref[lead + core, rows:, :] = end
                else:
                    @pl.when(first > 0)
                    def _():
                        lead = 2 * ring_place(jnp.maximum(first // 2 - 1, 0), slabs // 2)
                        out_ref[lead + core, rows:, :] = end
        for far, block in enumerate(late):
            carry[far] = block
        return 0

    if run == slabs:
        turn(0, 0)
    else:
        lax.fori_loop(0, slabs // run, turn, 0)


def band_stage(filterbank, chan_delay, slabs):
    groups = chan_delay.shape[0]
    channels, samples = filterbank.shape
    rows = channels // SUBCH * groups
    run = math.gcd(slabs, 16)
    return pl.pallas_call(
        functools.partial(band_kernel, channels // SUBCH, groups, run),
        out_shape=jax.ShapeDtypeStruct((slabs, rows + rows // 8, LANES), jnp.bfloat16),
        in_specs=[pl.BlockSpec(memory_space=pltpu.HBM)] * 2,
        scratch_shapes=[
            pltpu.VMEM((channels, samples + LANES), jnp.bfloat16),
            pltpu.VMEM(chan_delay.shape, jnp.int32),
            pltpu.VMEM((DELAY_ONE // NEAR - 1, rows, LANES), jnp.float32),
            pltpu.VMEM((run * rows // 2, LANES), jnp.float32),
            pltpu.SemaphoreType.DMA((FETCHES + 1,)),
        ],
        compiler_params=pltpu.CompilerParams(
            vmem_limit_bytes=(8 << 20) + 2 * filterbank.size,
        ),
        name="bands",
    )(*(pltpu.with_memory_space_constraint(x, pltpu.HBM) for x in (filterbank, chan_delay)))


def group_lanes(block_rows, group, per_group):
    start = group * per_group
    first, shift = start // LANES, start % LANES
    front = block_rows(first)
    if shift + per_group <= LANES:
        return front
    lane = lax.broadcasted_iota(jnp.int32, front.shape, 1)
    return jnp.where(lane < shift, block_rows(first + 1), front)


def one_hot(delays, first, count):
    return jnp.concatenate([jnp.where(delays == first + e, 1.0, 0.0) for e in range(count)], 0)


def pieces_of(per_group):
    period = per_group // HALO
    starts = [LANES * m // per_group for m in range(period)]
    splits = [per_group * (g + 1) - LANES * m for m, g in enumerate(starts)]
    return period, starts, splits


def series_kernel(whole, per_group, held_ref, delay_ref, series_ref, stat_ref, wide, slid, dense, near, rows_at):
    sources, row_count, _ = held_ref.shape
    groups = series_ref.shape[0]
    bands, trials = delay_ref.shape
    per_source = bands // sources
    part = per_source * groups
    blocks = trials // 2 // LANES
    pitch = row_count + 1
    copies = max(1, LANES // bands)
    slab = 2 * LANES
    span = slab + WMAX
    base = 8
    lead = lax.axis_index("core") * blocks
    for block in range(blocks):
        at = pl.multiple_of((lead + block) * LANES, LANES)
        dense[block] = delay_ref[:, pl.ds(at, LANES)]

    def ordered(block):
        return jnp.concatenate(
            [dense[block, pl.ds(b, sources, per_source), :] for b in range(per_source)], 0
        )

    for group in range(groups):
        near[group] = group_lanes(ordered, group, per_group)
    for source in range(sources):
        came = 2 * ring_place(source // 2, sources // 2) + source % 2
        wide[source * pitch : source * pitch + row_count, :] = held_ref[came].astype(jnp.float32)

    def turned(first_row, stride):
        picked = [
            wide[pl.ds(first_row + b * stride, sources, pitch), :] for b in range(per_source)
        ]
        return jnp.concatenate(picked * copies, 0).T

    def store(q, first, block):
        slid[q, base + first : base + first + block.shape[0], :] = block

    def store_slid(q, first, block):
        for copy in range(1, copies):
            low = copy * bands
            top = low + bands
            begin = base + first - copy
            slid[q, begin : begin + block.shape[0], low:top] = block[:, low:top]

    def quad_of(quad, at):
        tails = turned(2 * part + quad, groups // 4)
        for q in range(4):
            group = quad * 4 + q
            place = at + q
            pieces = [turned(side * part + group, groups) for side in range(2)]
            pieces.append(tails[q * HALO : (q + 1) * HALO])
            for side, piece in enumerate(pieces):
                store(place, side * LANES, piece)
            for side, piece in enumerate(pieces):
                store_slid(place, side * LANES, piece)
            both = jnp.zeros((span + FAR, 2 * LANES), jnp.float32)
            step = 2 * copies
            for offset in range(0, FAR, step):
                hot = jnp.concatenate(
                    [one_hot(near[group], far + offset, step) for far in (0, FAR)], 1
                )
                left = jnp.concatenate(
                    [
                        slid[place, base + o : base + o + span + FAR, :]
                        for o in range(offset, offset + step, copies)
                    ],
                    1,
                )
                both = both + jnp.dot(left, hot, preferred_element_type=jnp.float32)
            out = both[:span, :LANES] + both[FAR:, LANES:]
            series_ref[group] = out
            own = out[:slab]
            total = jnp.sum(own, 0, keepdims=True)
            centred = own - total * (1.0 / slab)
            rows_at[0, pl.ds(group, 1), :] = total
            rows_at[1, pl.ds(group, 1), :] = jnp.sum(centred * centred, 0, keepdims=True)

    if whole:
        for quad in range(groups // 4):
            quad_of(quad, quad * 4)
    else:

        def turn(quad, _):
            quad_of(quad, 0)
            return 0

        lax.fori_loop(0, groups // 4, turn, 0)

    period, starts, splits = pieces_of(per_group)
    cycle = period + 1
    lane = lax.broadcasted_iota(jnp.int32, (groups // cycle, LANES), 1)
    packed = []
    for stat in range(2):
        moved = [rows_at[stat, pl.ds(q, groups // cycle, cycle), :] for q in range(cycle)]
        for start, split in zip(starts, splits):
            packed.append(jnp.where(lane < split, moved[start], moved[start + 1]))
    stat_ref[...] = jnp.concatenate(packed, 0)


def series_stage(held, delays, groups):
    sources, row_count, _ = held.shape
    bands, trials = delays.shape
    across = max(LANES, bands)
    whole = bands <= LANES
    half = groups // 2
    return pl.pallas_call(
        functools.partial(series_kernel, whole, trials // groups),
        out_shape=(
            jax.ShapeDtypeStruct((half, 2 * LANES + WMAX, LANES), jnp.float32),
            jax.ShapeDtypeStruct((trials // LANES, LANES), jnp.float32),
        ),
        scratch_shapes=[
            pltpu.VMEM((sources * (row_count + 1) + 7, LANES), jnp.float32),
            pltpu.VMEM((half if whole else 4, 2 * LANES + HALO + 8, across), jnp.float32),
            pltpu.VMEM((trials // 2 // LANES, bands, LANES), jnp.int32),
            pltpu.VMEM((half, bands, LANES), jnp.int32),
            pltpu.VMEM((2, half, LANES), jnp.float32),
        ],
        compiler_params=pltpu.CompilerParams(
            vmem_limit_bytes=(8 << 20) + (0 if whole else 32 << 20),
        ),
        name="series",
    )(held, delays)


def box_kernel(per_group, series_ref, width_ref, keep_ref, send_ref, pairs, ones, fours, threes):
    groups = series_ref.shape[0]
    slab = 2 * LANES
    period, starts, splits = pieces_of(per_group)
    cycle = period + 1
    blocks = keep_ref.shape[0]
    core = lax.axis_index("core")
    lane = lax.broadcasted_iota(jnp.int32, (LANES, LANES), 1)

    def window(ref, group, first, count):
        return ref[group, first : first + count, :]

    def boxes(group):
        width = group_lanes(
            lambda r: width_ref[pl.ds(core * blocks + r, 1), :], group, per_group
        )
        bits = [width & (1 << e) > 0 for e in range(5)]
        top = slab + 15
        here = window(series_ref, group, 0, top)
        pairs[group, :top, :] = here + window(series_ref, group, 1, top)
        ones[group, :top, :] = jnp.where(bits[0], here, 0.0)
        top = slab + 12
        two = window(pairs, group, 0, top)
        fours[group, :top, :] = two + window(pairs, group, 2, top)
        threes[group, :top, :] = jnp.where(
            bits[1], two + window(ones, group, 2, top), window(ones, group, 0, top)
        )
        sides = []
        for side in range(0, slab, LANES):
            top = LANES + 8
            four = window(fours, group, side, top)
            eight = four + window(fours, group, side + 4, top)
            seven = jnp.where(
                bits[2],
                four + window(threes, group, side + 4, top),
                window(threes, group, side, top),
            )
            some = jnp.where(bits[3], eight[:LANES] + seven[8:], seven[:LANES])
            sides.append(jnp.where(bits[4], eight[:LANES] + eight[8:], some))
        return sides

    for turn in range(groups // cycle):
        moved = [boxes(turn * cycle + q) for q in range(cycle)]
        for j, (start, split) in enumerate(zip(starts, splits)):
            early, late = (
                jnp.where(lane < split, moved[start][side], moved[start + 1][side])
                for side in range(2)
            )
            keep_ref[turn * period + j] = jnp.where(core == 0, early, late)
            send_ref[turn * period + j] = jnp.where(core == 0, late, early)


def box_stage(series, widths, per_group):
    blocks = widths.shape[0] // 2
    return pl.pallas_call(
        functools.partial(box_kernel, per_group),
        out_shape=[jax.ShapeDtypeStruct((blocks, LANES, LANES), jnp.float32)] * 2,
        scratch_shapes=[pltpu.VMEM(series.shape, jnp.float32)] * 4,
        compiler_params=pltpu.CompilerParams(vmem_limit_bytes=12 << 20),
        cost_estimate=COST,
        name="box",
    )(series, widths)


def pair_kernel(own_ref, other_ref, out_ref):
    half = own_ref.shape[0] // 2
    own, other = own_ref[...], other_ref[...]
    first = lax.axis_index("core") == 0
    low = jnp.where(first, own, other)
    high = jnp.where(first, other, own)
    both = jnp.concatenate([low[:half], high[:half], low[half:], high[half:]], 0)
    out_ref[...] = jnp.broadcast_to(both[None], out_ref.shape)


def pair_stage(own, other, peers):
    return pl.pallas_call(
        pair_kernel,
        out_shape=jax.ShapeDtypeStruct((peers, 2 * own.shape[0], LANES), jnp.float32),
        compiler_params=pltpu.CompilerParams(vmem_limit_bytes=8 << 20),
        name="pair",
    )(own, other)


def snr_kernel(samples, period, keep_ref, came_ref, stat_ref, width_ref, out_hbm, done, levels, sems):
    sources, stat_rows, _ = stat_ref.shape
    blocks = stat_rows // 2
    half = blocks // 2
    turns = half // period
    own = samples // sources
    totals = stat_ref[:, :blocks, :]
    average = jnp.sum(totals, 0) * (1.0 / samples)
    apart = totals * (1.0 / own) - average[None]
    squares = jnp.sum(stat_ref[:, blocks:, :], 0) + own * jnp.sum(apart * apart, 0)
    variance = squares * (1.0 / samples)
    width = jnp.concatenate(
        [width_ref[pl.ds(c * half + j, turns, period), :] for c in range(2) for j in range(period)], 0
    )
    width = width.astype(jnp.float32)
    levels[0] = width * average
    levels[1] = lax.rsqrt(width * (variance + 1e-05))
    core = lax.axis_index("core")
    copies = []
    for order, (box_ref, place) in enumerate(((keep_ref, core), (came_ref, 1 - core))):
        for block in range(half):
            row = place * half + block % period * turns + block // period
            at = order * half + block
            level = levels[0, pl.ds(row, 1), :]
            scale = levels[1, pl.ds(row, 1), :]
            done[at * LANES : (at + 1) * LANES, :] = ((box_ref[block] - level) * scale).T
            if (block + 1) % OUT_BLOCKS == 0:
                size = OUT_BLOCKS * LANES
                target = pl.multiple_of((place * half + block + 1 - OUT_BLOCKS) * LANES, LANES)
                copy = pltpu.make_async_copy(
                    done.at[(at + 1) * LANES - size : (at + 1) * LANES, :],
                    out_hbm.at[pl.ds(target, size), :],
                    sems.at[at // OUT_BLOCKS],
                )
                copy.start()
                copies.append(copy)
    for copy in copies:
        copy.wait()


def snr_stage(keep, came, stats, widths, samples, period):
    blocks = widths.shape[0]
    return pl.pallas_call(
        functools.partial(snr_kernel, samples, period),
        out_shape=jax.ShapeDtypeStruct((blocks * LANES, LANES), jnp.float32),
        out_specs=pl.BlockSpec(memory_space=pltpu.HBM),
        scratch_shapes=[
            pltpu.VMEM((blocks * LANES, LANES), jnp.float32),
            pltpu.VMEM((2, blocks, LANES), jnp.float32),
            pltpu.SemaphoreType.DMA((blocks // OUT_BLOCKS,)),
        ],
        compiler_params=pltpu.CompilerParams(vmem_limit_bytes=8 << 20),
        name="snr",
    )(keep, came, stats, widths)


def per_device(filterbank, chan_delay, sub_delay, widths):
    samples = filterbank.shape[1]
    groups = chan_delay.shape[0]
    per_group = sub_delay.shape[0] // groups
    chips, cores = lax.axis_size("chip"), lax.axis_size("core")
    widths = widths.reshape(-1, LANES)
    sent = band_stage(filterbank, chan_delay, chips * cores)
    held = lax.all_to_all(
        sent,
        ("chip", "core"),
        split_axis=0,
        concat_axis=0,
        tiled=True,
        axis_index_groups=[ring_of(chips, cores)],
    )
    series, stats = series_stage(held, sub_delay.T, groups)
    swap = [(0, 1), (1, 0)]
    other = lax.ppermute(stats, "core", swap)
    keep, send = box_stage(series, widths, per_group)
    other, send = lax.optimization_barrier((other, send))
    came = lax.ppermute(send, "core", swap)
    stats = pair_stage(stats, other, chips)
    stats = lax.all_to_all(
        stats,
        "chip",
        split_axis=0,
        concat_axis=0,
        tiled=True,
    )
    return snr_stage(keep, came, stats, widths, samples, pieces_of(per_group)[0])


def solution(mesh):
    beams, devices = mesh.devices.shape
    split = jax.sharding.Mesh(
        mesh.devices.reshape(beams, devices // 2, 2), ("beam", "chip", "core")
    )
    lines = ("chip", "core")
    in_specs = (P(("beam", *lines), None), P(None, lines), P(), P())
    out_specs = P("beam", lines)
    return jax.shard_map(
        per_device, mesh=split, in_specs=in_specs, out_specs=out_specs, check_vma=False
    )
```
